256 devices in a mesh: grp: 2 (over z), scen: 128 (over x, y, core).
Axes of the slice: x: 8, y: 8, z: 2, core: 2. Of those that a mesh axis runs over, the one named last changes fastest.
The devices are a block of a 8x8x16 slice.
Arguments:
- shocks: bfloat16 [262144, 2048], P(('grp', 'scen')), parts along dimension 0, may hold values from -8 to 8
- factor_sens: bfloat16 [2048, 1024], replicated, may hold values from -0.13258252 to 0.13258252
- notional: float32 [1024], replicated, may hold values from -0.25 to 0.25
- moneyness: float32 [1024], replicated, may hold values from -2 to 2
- desk_entity: int32 [64], replicated, may hold values from 0 to 7
- scenario_counts: int32 [256], P(('grp', 'scen')), parts along dimension 0, may hold values from 256 to 1024, as said below
- candidate_ids: int32 [2048], P('grp'), parts along dimension 0, may hold values from 0 to 131071, as said below
Outputs:
- tail_losses: float32 [512], P('grp'), parts along dimension 0
- cand_entity: float32 [2048, 8], P(('grp', 'scen')), parts along dimension 0
The draws below stay inside these ranges and needn't reach their ends.
There are 2 independent parts, one for each index of `grp`. The reference program is written for one: setup_inputs(seed, part) draws one part's arguments, and reference() takes and returns one part's arrays. A program takes and returns all parts, laid end to end along the dimension named above; an argument that names none is the same for every part. Nothing has to cross between parts.
Inputs may be any that keep to these rules, and one draw needn't show every extreme that they name: `scenario_counts`: every block has at least 256 valid scenarios; some block in every draw is full. `candidate_ids`: each id b * 1024 + j names a valid scenario: j is below scenario_counts[b].
All inputs are finite; a program needn't handle non-finite values.
Results may differ from the reference program's by a relative error of at most 0.0003.
Values sent between devices are 32-bit elements; how exact they have to be, the bound alone decides.
No kernel may reach another device: no remote copies, remote signals or barrier semaphores. Data moves between devices by JAX's collectives and lax.ppermute only.
A program may use at most 128 MiB of HBM per device.

```python
import jax
import jax.numpy as jnp
from jax import lax

F = 2048
K = 64
INSTR = 16
ENT = 8
TOPK = 256
CAND = 1024
S_DEV = 1024
N_SCEN = 128


def common_draw(key):
    base = jax.random.fold_in(key, 7)
    key_a, key_b, key_c, key_d = jax.random.split(base, 4)
    counts = jax.random.randint(key_a, (N_SCEN,), S_DEV // 4, S_DEV + 1)
    filled = jax.random.randint(key_b, (), 0, N_SCEN)
    counts = jnp.where(jnp.arange(N_SCEN) == filled, S_DEV, counts).astype(jnp.int32)
    owners = jax.random.randint(key_c, (CAND,), 0, N_SCEN)
    offsets = jax.random.randint(key_d, (CAND,), 0, counts[owners])
    return (counts, (owners * S_DEV + offsets).astype(jnp.int32), filled)


def draw_scenario_counts(key, part):
    return common_draw(key)[0]


def draw_candidate_ids(key, part):
    return common_draw(key)[1]


def draw_shocks(key, part):
    filled = common_draw(key)[2]
    noise_key = jax.random.fold_in(key, 11)
    moves = jax.random.normal(noise_key, (S_DEV * N_SCEN, F), jnp.float32)
    hot_scale = 2.0
    block_of_row = jnp.arange(S_DEV * N_SCEN, dtype=jnp.int32) // S_DEV
    scales = jnp.where(block_of_row == filled, jnp.float32(hot_scale), jnp.float32(1.0))
    return jnp.clip(moves * scales[:, None], -8.0, 8.0).astype(jnp.bfloat16)


def draw_factor_sens(key, part):
    half = K * INSTR // 2
    key_a, key_b = jax.random.split(jax.random.fold_in(key, 21))
    first = jnp.clip(jax.random.normal(key_a, (F, half), jnp.float32), -4.0, 4.0)
    second = jnp.clip(jax.random.normal(key_b, (F, half), jnp.float32), -4.0, 4.0)
    paired = jnp.stack([first, -first + 0.15 * second], axis=2).reshape(F, K * INSTR)
    return (paired * F ** (-0.5)).astype(jnp.bfloat16)


def draw_notional(key, part):
    half = K * INSTR // 2
    scale = 2.0 * (K * INSTR) ** (-0.5)
    noise_key = jax.random.fold_in(key, 31)
    values = jnp.clip(jax.random.normal(noise_key, (half,), jnp.float32), -4.0, 4.0)
    return jnp.repeat(values * scale, 2).astype(jnp.float32)


def draw_moneyness(key, part):
    half = K * INSTR // 2
    noise_key = jax.random.fold_in(key, 41)
    values = jax.random.uniform(noise_key, (half,), jnp.float32, -2.0, 2.0)
    return jnp.repeat(values, 2).astype(jnp.float32)


def set_ends(entries, stream_key, least, top_value):
    longest = entries.shape.index(max(entries.shape))
    spots = []
    for shift in (0, 1):
        where = [jax.random.randint(jax.random.fold_in(stream_key, axis), (), 0, length) for axis, length in enumerate(entries.shape)]
        where[longest] = (where[longest] + shift) % entries.shape[longest]
        spots.append(tuple(where))
    return entries.at[spots[0]].set(least).at[spots[1]].set(top_value)


def setup_inputs(seed: int = 0, part: int = 0) -> dict:
    arg_keys = jax.random.split(jax.random.key(seed), 8)
    part_keys = jax.random.split(jax.random.fold_in(arg_keys[7], part), 8)
    shocks = draw_shocks(jax.random.fold_in(jax.random.fold_in(arg_keys[7], part), 71), part)
    factor_sens = draw_factor_sens(jax.random.fold_in(arg_keys[7], 71), part)
    notional = draw_notional(jax.random.fold_in(arg_keys[7], 71), part)
    moneyness = draw_moneyness(jax.random.fold_in(arg_keys[7], 71), part)
    desk_entity = set_ends(jax.random.randint(arg_keys[4], (K,), 0, ENT), jax.random.fold_in(arg_keys[4], 1), 0, ENT - 1).astype(jnp.int32)
    scenario_counts = draw_scenario_counts(jax.random.fold_in(jax.random.fold_in(arg_keys[7], part), 71), part)
    candidate_ids = draw_candidate_ids(jax.random.fold_in(jax.random.fold_in(arg_keys[7], part), 71), part)
    return {"shocks": shocks, "factor_sens": factor_sens, "notional": notional, "moneyness": moneyness, "desk_entity": desk_entity, "scenario_counts": scenario_counts, "candidate_ids": candidate_ids}


def price(rows, factor_sens, notional, moneyness):
    value = jnp.dot(rows, factor_sens, preferred_element_type=jnp.float32)
    inst = notional * (jax.nn.softplus(value + moneyness) - jax.nn.softplus(moneyness))
    return jnp.sum(inst.reshape(rows.shape[0], K, INSTR), axis=2)


def reference(shocks, factor_sens, notional, moneyness, desk_entity, scenario_counts, candidate_ids):
    blocks = shocks.reshape(N_SCEN, S_DEV, F)

    def one_block(item):
        rows, count = item
        loss = -jnp.sum(price(rows, factor_sens, notional, moneyness), axis=1)
        valid = jnp.arange(S_DEV, dtype=jnp.int32) < count
        return jnp.where(valid, loss, jnp.float32(-1e30))

    losses = lax.map(one_block, (blocks, scenario_counts))
    tail_losses = lax.top_k(losses.reshape(-1), TOPK)[0]
    cand_rows = jnp.take(shocks, candidate_ids, axis=0)
    cand_pnl = price(cand_rows, factor_sens, notional, moneyness)
    onehot = (desk_entity[:, None] == jnp.arange(ENT, dtype=jnp.int32)[None, :]).astype(jnp.float32)
    cand_entity = -jnp.dot(cand_pnl, onehot, precision=lax.Precision.HIGHEST)
    return tail_losses, cand_entity
```

```python
import functools

import jax
import jax.numpy as jnp
from jax import lax
from jax.experimental import pallas as pl
from jax.experimental.pallas import tpu as pltpu
from jax.sharding import PartitionSpec as P

K = 64
INSTR = 16
ENT = 8
TOPK = 256
LANES = 128
LOG2E = 1.4426950408889634
LN2 = 0.6931471805599453
LOW = -1e30

VMEM = pl.BlockSpec(memory_space=pltpu.VMEM)
SMEM = pl.BlockSpec(memory_space=pltpu.SMEM)
ANY = pl.BlockSpec(memory_space=pl.ANY)


def softplus2(t):
    return jnp.maximum(t, 0.0) + jnp.log2(1.0 + jnp.exp2(-jnp.abs(t)))


def iota(shape, dim):
    return lax.broadcasted_iota(jnp.int32, shape, dim)


def split_bf16(x):
    hi = x.astype(jnp.bfloat16)
    return hi, (x - hi.astype(jnp.float32)).astype(jnp.bfloat16)


def price_kernel(
    axis, devices, count_ref, desk_ref, ids_ref, notional_ref, money_ref, shocks_hbm, sens_hbm,
    out_ref, rows_ref, sens_ref, ent_w, res_ref, pick_ref, idc_ref, row_sems, sens_sems,
):
    slots, factors = rows_ref.shape
    instruments = sens_ref.shape[1]
    cands = ids_ref.shape[1]
    step = 256
    blocks = slots // step
    parts = instruments // step

    def row_copy(i):
        part = pl.ds(i * step, step)
        return pltpu.make_async_copy(shocks_hbm.at[part], rows_ref.at[part], row_sems.at[i])

    def sens_copy(j):
        part = pl.ds(j * step, step)
        return pltpu.make_async_copy(sens_hbm.at[:, part], sens_ref.at[:, part], sens_sems.at[j])

    row_copy(0).start()
    sens_copy(0).start()
    for j in range(1, parts):
        sens_copy(j).start()
    for i in range(1, blocks):
        row_copy(i).start()

    me = lax.axis_index(axis)
    lane = iota((INSTR, LANES), 1)
    for k in range(K):
        hit = (lane & (ENT - 1)) == desk_ref[k]
        ent_w[pl.ds(k * INSTR, INSTR), 0:LANES] = jnp.where(hit, -1.0, 0.0).astype(jnp.bfloat16)
    ent_w[:, LANES:] = jnp.full((instruments, LANES), -1.0, jnp.bfloat16)
    money = money_ref[...] * LOG2E
    base = softplus2(money)
    scale = notional_ref[...] * LN2
    local = (ids_ref[...] - me * slots).astype(jnp.float32)
    for b in range(cands // LANES):
        span = pl.ds(b * LANES, LANES)
        row = jnp.broadcast_to(local[:, b * LANES : (b + 1) * LANES], (LANES, LANES))
        idc_ref[span, :] = jnp.transpose(row)

    def tile(i, j):
        cols = slice(j * step, (j + 1) * step)
        rows = pl.ds(i * step, step)
        value = jnp.dot(rows_ref[rows, :], sens_ref[:, cols], preferred_element_type=jnp.float32)
        inst = scale[:, cols] * (softplus2(value * LOG2E + money[:, cols]) - base[:, cols])
        hi, lo = split_bf16(inst)
        w = ent_w[cols, :]
        return jnp.dot(hi, w, preferred_element_type=jnp.float32) + jnp.dot(
            lo, w, preferred_element_type=jnp.float32
        )

    def finish(i, total):
        res_ref[pl.ds(i * step, step), :] = total
        width = cands // blocks
        mine = pl.ds(i * width, width)
        want = idc_ref[mine, :]
        spot = iota((width, LANES), 1).astype(jnp.float32)
        for b in range(slots // LANES):
            hit = want == spot + float(b * LANES)
            pick_ref[mine, b * LANES : (b + 1) * LANES] = jnp.where(hit, 1.0, 0.0).astype(
                jnp.bfloat16
            )

    row_copy(0).wait()
    total = None
    for j in range(parts):
        sens_copy(j).wait()
        piece = tile(0, j)
        total = piece if total is None else total + piece
    finish(0, total)

    def one_block(i, carry):
        row_copy(i).wait()
        whole = tile(i, 0)
        for j in range(1, parts):
            whole = whole + tile(i, j)
        finish(i, whole)
        return carry

    lax.fori_loop(1, blocks, one_block, 0)

    ent_hi, ent_lo = split_bf16(res_ref[:, 0:LANES])
    both = jnp.concatenate([ent_hi, ent_lo], axis=1)
    got = jnp.dot(pick_ref[...], both, preferred_element_type=jnp.float32)
    got = got[:, 0:LANES] + got[:, LANES:]
    per = cands // devices
    got = got.reshape(devices, per, LANES)
    keep = iota((1, per, LANES), 2) // ENT == iota((1, per, LANES), 1)
    out_ref[:, :, TOPK:] = jnp.sum(jnp.where(keep, got, 0.0), axis=1, keepdims=True)

    count = count_ref[0]
    col = jnp.where(iota((slots, LANES), 0) < count, res_ref[:, LANES:], LOW)
    eye = iota((LANES, LANES), 0) == iota((LANES, LANES), 1)
    before = iota((LANES, LANES), 1) < iota((LANES, LANES), 0)
    acc = [jnp.zeros((LANES, LANES), jnp.float32) for _ in range(slots // LANES)]
    for b in range(slots // LANES):
        here = col[b * LANES : (b + 1) * LANES]
        row = jnp.sum(jnp.where(eye, here, 0.0), axis=0, keepdims=True)
        row = jnp.broadcast_to(row, (LANES, LANES))
        for a in range(slots // LANES):
            mine = col[a * LANES : (a + 1) * LANES]
            if b < a:
                ahead = row >= mine
            elif b > a:
                ahead = row > mine
            else:
                ahead = (row > mine) | ((row == mine) & before)
            acc[a] = acc[a] + jnp.where(ahead, 1.0, 0.0)
    ahead = jnp.concatenate(acc, axis=0).astype(jnp.bfloat16)
    rank = jnp.dot(ahead, jnp.ones((LANES, LANES), jnp.bfloat16), preferred_element_type=jnp.float32)
    rising = me >= devices // 2
    for h in range(TOPK // LANES):
        place = iota((slots, LANES), 1) + h * LANES
        place = jnp.where(rising, TOPK - 1 - place, place).astype(jnp.float32)
        line = jnp.sum(jnp.where(rank == place, col, 0.0), axis=0, keepdims=True)
        out_ref[:, :, h * LANES : (h + 1) * LANES] = jnp.broadcast_to(
            line[None], (devices, 1, LANES)
        )


def merge_kernel(in_ref, tail_ref, cand_ref):
    devices = in_ref.shape[0]
    lists = in_ref[...].reshape(devices, in_ref.shape[2])
    sums = jnp.sum(lists[:, TOPK:], axis=0, keepdims=True)
    spread = jnp.where(iota((8, LANES), 1) // ENT == iota((8, LANES), 0), sums, 0.0)
    for d in (32, 16, 8):
        spread = spread + pltpu.roll(spread, LANES - d, 1)
    cand_ref[...] = spread[:, 0:ENT]

    turned = [jnp.transpose(lists[:, h * LANES : (h + 1) * LANES]) for h in range(TOPK // LANES)]
    per = LANES // 8
    x = [turned[g // per][8 * (g % per) : 8 * (g % per) + 8] for g in range(TOPK // 8)]
    lane = iota((8, LANES), 1)
    sub = iota((8, LANES), 0)

    def ordered(x):
        gap = len(x) // 2
        while gap:
            new = list(x)
            for g in range(len(x)):
                if not g & gap:
                    new[g] = jnp.maximum(x[g], x[g + gap])
                    new[g + gap] = jnp.minimum(x[g], x[g + gap])
            x, gap = new, gap // 2
        for gap in (4, 2, 1):
            upper = (sub & gap) == 0
            new = []
            for v in x:
                other = pltpu.roll(v, 8 - gap, 0)
                low = pltpu.roll(jnp.minimum(v, other), gap, 0)
                new.append(jnp.where(upper, jnp.maximum(v, other), low))
            x = new
        return x

    gap = devices // 2
    while gap:
        x = [jnp.maximum(v, pltpu.roll(v, gap, 1)) for v in x]
        gap //= 2
        if gap:
            sign = jnp.where((lane & gap) == 0, 1.0, -1.0)
            x = [v * sign for v in ordered([v * sign for v in x])]
    x = ordered(x)
    eye = iota((LANES, LANES), 0) == iota((LANES, LANES), 1)
    for h in range(TOPK // LANES):
        block = jnp.concatenate(x[h * per : (h + 1) * per], axis=0)
        tail_ref[:, h * LANES : (h + 1) * LANES] = jnp.sum(
            jnp.where(eye, block, 0.0), axis=0, keepdims=True
        )


def body(axis, shocks, factor_sens, notional, moneyness, desk_entity, scenario_counts, candidate_ids):
    slots, factors = shocks.shape
    instruments = factor_sens.shape[1]
    cands = candidate_ids.shape[0]
    devices = lax.axis_size(axis)
    width = TOPK + LANES
    sent = pl.pallas_call(
        functools.partial(price_kernel, axis, devices),
        out_shape=jax.ShapeDtypeStruct((devices, 1, width), jnp.float32),
        in_specs=[SMEM, SMEM, VMEM, VMEM, VMEM, ANY, ANY],
        out_specs=VMEM,
        scratch_shapes=[
            pltpu.VMEM((slots, factors), jnp.bfloat16),
            pltpu.VMEM((factors, instruments), jnp.bfloat16),
            pltpu.VMEM((instruments, 2 * LANES), jnp.bfloat16),
            pltpu.VMEM((slots, 2 * LANES), jnp.float32),
            pltpu.VMEM((cands, slots), jnp.bfloat16),
            pltpu.VMEM((cands, LANES), jnp.float32),
            pltpu.SemaphoreType.DMA((slots // 256,)),
            pltpu.SemaphoreType.DMA((instruments // 256,)),
        ],
        name="price",
    )(
        scenario_counts,
        desk_entity,
        candidate_ids.reshape(1, cands),
        notional.reshape(1, instruments),
        moneyness.reshape(1, instruments),
        shocks,
        factor_sens,
    )
    got = lax.all_to_all(sent, axis, 0, 0, tiled=True)
    tail, cand = pl.pallas_call(
        merge_kernel,
        out_shape=[
            jax.ShapeDtypeStruct((1, TOPK), jnp.float32),
            jax.ShapeDtypeStruct((cands // devices, ENT), jnp.float32),
        ],
        in_specs=[VMEM],
        out_specs=[VMEM, VMEM],
        name="merge",
    )(got)
    return tail.reshape(TOPK), cand


def solution(mesh):
    return jax.shard_map(
        functools.partial(body, "scen"),
        mesh=mesh,
        in_specs=(P(("grp", "scen"), None), P(), P(), P(), P(), P(("grp", "scen")), P("grp")),
        out_specs=(P("grp"), P(("grp", "scen"), None)),
        check_vma=False,
    )
```

```python
import functools

import jax
import jax.numpy as jnp
from jax import lax
from jax.experimental import pallas as pl
from jax.experimental.pallas import tpu as pltpu
from jax.sharding import PartitionSpec as P

K = 64
INSTR = 16
ENT = 8
TOPK = 256
LANES = 128
LOG2E = 1.4426950408889634
LN2 = 0.6931471805599453
LOW = -1e30

VMEM = pl.BlockSpec(memory_space=pltpu.VMEM)
SMEM = pl.BlockSpec(memory_space=pltpu.SMEM)
HBM = pl.BlockSpec(memory_space=pltpu.HBM)
PRICE_VMEM = 24 << 20
MERGE_VMEM = 8 << 20


def softplus2(t):
    return jnp.maximum(t, 0.0) + jnp.log2(1.0 + jnp.exp2(-jnp.abs(t)))


def iota(shape, dim):
    return lax.broadcasted_iota(jnp.int32, shape, dim)


def split_bf16(x):
    hi = x.astype(jnp.bfloat16)
    return hi, (x - hi.astype(jnp.float32)).astype(jnp.bfloat16)


def price_kernel(
    axis, devices, count_ref, desk_hbm, ids_hbm, notional_hbm, money_hbm, shocks_hbm, sens_hbm,
    out_ref, rows_ref, sens_ref, ent_w, res_ref, pick_ref, idc_ref, halves_ref, ids_ref, notional_ref,
    money_ref, base_ref, desk_ref, row_sems, sens_sems, small_sems,
):
    slots, factors = rows_ref.shape
    instruments = sens_ref.shape[1]
    cands = ids_ref.shape[1]
    step = 256
    blocks = slots // step
    pairs = instruments // (2 * step)
    deep = factors // step
    ch = 64
    chunks = step // ch
    mxus = (0, 1)

    def row_copy(i):
        part = pl.ds(i * step, step)
        return pltpu.make_async_copy(shocks_hbm.at[part], rows_ref.at[part], row_sems.at[i])

    def sens_copy(p):
        part = pl.ds(p * 2 * step, 2 * step)
        return pltpu.make_async_copy(sens_hbm.at[:, part], sens_ref.at[:, part], sens_sems.at[p])

    small = [
        pltpu.make_async_copy(a, b, small_sems.at[n])
        for n, (a, b) in enumerate(
            (
                (desk_hbm, desk_ref),
                (ids_hbm, ids_ref),
                (notional_hbm, notional_ref),
                (money_hbm, money_ref),
            )
        )
    ]
    for copy in small:
        copy.start()
    row_copy(0).start()
    for p in range(pairs):
        sens_copy(p).start()
    for i in range(1, blocks):
        row_copy(i).start()
    for copy in small:
        copy.wait()

    me = lax.axis_index(axis)
    lane = iota((INSTR, LANES), 1)
    for k in range(K):
        hit = (lane & (ENT - 1)) == desk_ref[k]
        ent_w[pl.ds(k * INSTR, INSTR), 0:LANES] = jnp.where(hit, -1.0, 0.0).astype(jnp.bfloat16)
    ent_w[:, LANES:] = jnp.full((instruments, LANES), -1.0, jnp.bfloat16)
    money_ref[...] = money_ref[...] * LOG2E
    base_ref[...] = softplus2(money_ref[...])
    notional_ref[...] = notional_ref[...] * LN2
    local = (ids_ref[...] - me * slots).astype(jnp.float32)
    for b in range(cands // LANES):
        span = pl.ds(b * LANES, LANES)
        row = jnp.broadcast_to(local[:, b * LANES : (b + 1) * LANES], (LANES, LANES))
        idc_ref[span, :] = jnp.transpose(row)

    def main(accs):
        acc = {(q, m, c): accs[m][q * chunks + c] for q in mxus for m in mxus for c in range(chunks)}
        ent = {(m, c): accs[m][2 * chunks + c] for m in mxus for c in range(chunks)}

        def matmul(r, p, k):
            deep_k = slice(k * step, (k + 1) * step)
            for m in mxus:
                cols = slice((2 * p + m) * step, (2 * p + m + 1) * step)
                pltpu.matmul_push_rhs(sens_ref[deep_k, cols], 0, m)
            for c in range(chunks):
                at = pl.ds(pl.multiple_of(r * step, step) + c * ch, ch)
                lhs = rows_ref[at, deep_k]
                for m in mxus:
                    pltpu.matmul_acc_lhs(acc[p, m, c], lhs, 0 if c == 0 else None)

        def epilogue(p, m, c):
            cols = slice((2 * p + m) * step, (2 * p + m + 1) * step)
            value = pltpu.matmul_pop(acc[p, m, c])
            inst = notional_ref[:, cols] * (
                softplus2(value * LOG2E + money_ref[:, cols]) - base_ref[:, cols]
            )
            hi, lo = split_bf16(inst)
            halves_ref[m, 0, c * ch : (c + 1) * ch, :] = hi
            halves_ref[m, 1, c * ch : (c + 1) * ch, :] = lo

        def entities(p):
            for m in mxus:
                cols = slice((2 * p + m) * step, (2 * p + m + 1) * step)
                pltpu.matmul_push_rhs(ent_w[cols, :], 1, m)
            for h in range(2):
                for c in range(chunks):
                    for m in mxus:
                        part = halves_ref[m, h, c * ch : (c + 1) * ch, :]
                        pltpu.matmul_acc_lhs(ent[m, c], part, 1 if h + c == 0 else None)

        def collect(r):
            for c in range(chunks):
                at = pl.ds(pl.multiple_of(r * step, step) + c * ch, ch)
                res_ref[at, :] = pltpu.matmul_pop(ent[0, c]) + pltpu.matmul_pop(ent[1, c])

        def picks(i):
            width = cands // blocks
            mine = pl.ds(pl.multiple_of(i * width, width), width)
            want = idc_ref[mine, :]
            spot = iota((width, LANES), 1).astype(jnp.float32)
            for b in range(slots // LANES):
                hit = want == spot + float(b * LANES)
                pick_ref[mine, b * LANES : (b + 1) * LANES] = jnp.where(hit, 1.0, 0.0).astype(
                    jnp.bfloat16
                )

        def unit(r, p):
            last = 1 - p
            for k in range(deep):
                matmul(r, p, k)
                if k % 2 == 1 and k // 2 < chunks:
                    for m in mxus:
                        epilogue(last, m, k // 2)
                if p == 1 and k == 1:
                    collect(jnp.maximum(r - 1, 0))
            entities(last)

        def one_block(r, carry):
            row_copy(r).wait()

            @pl.when(r == 0)
            def _():
                sens_copy(0).wait()

            unit(r, 0)
            picks(r)

            @pl.when(r == 0)
            def _():
                sens_copy(1).wait()

            unit(r, 1)
            return carry

        lax.fori_loop(0, blocks, one_block, 0)
        for c in range(chunks):
            for m in mxus:
                epilogue(1, m, c)
        entities(1)
        collect(blocks - 1)

        per = cands // devices
        keep = iota((1, per, LANES), 2) // ENT == iota((1, per, LANES), 1)
        for k in range(slots // step):
            hi, lo = split_bf16(res_ref[k * step : (k + 1) * step, 0:LANES])
            both = jnp.concatenate([hi, lo], axis=1)
            for m in mxus:
                pltpu.matmul_push_rhs(both, k % 2, m)
            for c in range(2 * chunks):
                for m in mxus:
                    at = m * (cands // 2) + c * ch
                    lhs = pick_ref[at : at + ch, k * step : (k + 1) * step]
                    pltpu.matmul_acc_lhs(accs[m][c], lhs, k % 2 if c == 0 else None)

        groups = slots // LANES
        count = count_ref[0]
        col = jnp.where(iota((slots, LANES), 0) < count, res_ref[:, LANES:], LOW)
        eye = iota((LANES, LANES), 0) == iota((LANES, LANES), 1)
        before = iota((LANES, LANES), 1) < iota((LANES, LANES), 0)
        rows = []
        for b in range(groups):
            here = col[b * LANES : (b + 1) * LANES]
            row = jnp.sum(jnp.where(eye, here, 0.0), axis=0, keepdims=True)
            rows.append(jnp.broadcast_to(row, (LANES, LANES)))
        ones = jnp.ones((step, step), jnp.bfloat16)
        for m in mxus:
            pltpu.matmul_push_rhs(ones, 0, m)
        for a in range(groups):
            mine = col[a * LANES : (a + 1) * LANES]
            sums = []
            for half in range(2):
                acc_a = jnp.zeros((LANES, LANES), jnp.float32)
                for b in range(half * groups // 2, (half + 1) * groups // 2):
                    row = rows[b]
                    if b < a:
                        ahead = row >= mine
                    elif b > a:
                        ahead = row > mine
                    else:
                        ahead = (row > mine) | ((row == mine) & before)
                    acc_a = acc_a + jnp.where(ahead, 1.0, 0.0)
                sums.append(acc_a.astype(jnp.bfloat16))
            both = jnp.concatenate(sums, axis=1)
            m, a_m = a % 2, a // 2
            for c in range(2):
                pltpu.matmul_acc_lhs(
                    accs[m][2 * chunks + 2 * a_m + c],
                    both[c * ch : (c + 1) * ch],
                    0 if a_m + c == 0 else None,
                )
        for m in mxus:
            for c in range(2 * chunks):
                got = pltpu.matmul_pop(accs[m][c])
                got = (got[:, 0:LANES] + got[:, LANES:]).reshape(ch // per, per, LANES)
                at = (m * (cands // 2) + c * ch) // per
                out_ref[at : at + ch // per, :, TOPK:] = jnp.sum(
                    jnp.where(keep, got, 0.0), axis=1, keepdims=True
                )
        rising = me >= devices // 2
        lines = [jnp.zeros((ch, LANES), jnp.float32) for _ in range(TOPK // LANES)]
        spots = []
        for h in range(TOPK // LANES):
            place = iota((ch, LANES), 1) + h * LANES
            spots.append(jnp.where(rising, TOPK - 1 - place, place).astype(jnp.float32))
        for a in range(groups):
            for c in range(2):
                rank = pltpu.matmul_pop(accs[a % 2][2 * chunks + 2 * (a // 2) + c])[:, 0:LANES]
                at = a * LANES + c * ch
                for h in range(TOPK // LANES):
                    lines[h] = lines[h] + jnp.where(rank == spots[h], col[at : at + ch], 0.0)
        for h in range(TOPK // LANES):
            line = jnp.sum(lines[h], axis=0, keepdims=True)
            out_ref[:, :, h * LANES : (h + 1) * LANES] = jnp.broadcast_to(
                line[None], (devices, 1, LANES)
            )

    accs = [[pltpu.ACC(m)((ch, step), jnp.float32) for _ in range(4 * chunks)] for m in mxus]
    pl.run_scoped(lambda *refs: main((refs[: 4 * chunks], refs[4 * chunks :])), *accs[0], *accs[1])


def merge_kernel(in_ref, tail_ref, cand_ref):
    devices = in_ref.shape[0]
    lists = in_ref[...].reshape(devices, in_ref.shape[2])
    sums = jnp.sum(lists[:, TOPK:], axis=0, keepdims=True)
    spread = jnp.where(iota((8, LANES), 1) // ENT == iota((8, LANES), 0), sums, 0.0)
    for d in (32, 16, 8):
        spread = spread + pltpu.roll(spread, LANES - d, 1)
    cand_ref[...] = spread[:, 0:ENT]

    turned = [jnp.transpose(lists[:, h * LANES : (h + 1) * LANES]) for h in range(TOPK // LANES)]
    per = LANES // 8
    x = [turned[g // per][8 * (g % per) : 8 * (g % per) + 8] for g in range(TOPK // 8)]
    lane = iota((8, LANES), 1)
    sub = iota((8, LANES), 0)

    def ordered(x):
        gap = len(x) // 2
        while gap:
            new = list(x)
            for g in range(len(x)):
                if not g & gap:
                    new[g] = jnp.maximum(x[g], x[g + gap])
                    new[g + gap] = jnp.minimum(x[g], x[g + gap])
            x, gap = new, gap // 2
        for gap in (4, 2, 1):
            upper = (sub & gap) == 0
            new = []
            for v in x:
                other = pltpu.roll(v, 8 - gap, 0)
                low = pltpu.roll(jnp.minimum(v, other), gap, 0)
                new.append(jnp.where(upper, jnp.maximum(v, other), low))
            x = new
        return x

    gap = devices // 2
    while gap:
        x = [jnp.maximum(v, pltpu.roll(v, gap, 1)) for v in x]
        gap //= 2
        if gap:
            sign = jnp.where((lane & gap) == 0, 1.0, -1.0)
            x = [v * sign for v in ordered([v * sign for v in x])]
    x = ordered(x)
    eye = iota((LANES, LANES), 0) == iota((LANES, LANES), 1)
    for h in range(TOPK // LANES):
        block = jnp.concatenate(x[h * per : (h + 1) * per], axis=0)
        tail_ref[:, h * LANES : (h + 1) * LANES] = jnp.sum(
            jnp.where(eye, block, 0.0), axis=0, keepdims=True
        )


def price_call(slots, factors, instruments, cands, axis, devices):
    return pl.pallas_call(
        functools.partial(price_kernel, axis, devices),
        out_shape=jax.ShapeDtypeStruct((devices, 1, TOPK + LANES), jnp.float32),
        in_specs=[SMEM] + [HBM] * 6,
        out_specs=VMEM,
        scratch_shapes=[
            pltpu.VMEM((slots, factors), jnp.bfloat16),
            pltpu.VMEM((factors, instruments), jnp.bfloat16),
            pltpu.VMEM((instruments, 2 * LANES), jnp.bfloat16),
            pltpu.VMEM((slots, 2 * LANES), jnp.float32),
            pltpu.VMEM((cands, slots), jnp.bfloat16),
            pltpu.VMEM((cands, LANES), jnp.float32),
            pltpu.VMEM((2, 2, 256, 256), jnp.bfloat16),
            pltpu.VMEM((1, cands), jnp.int32),
            pltpu.VMEM((1, instruments), jnp.float32),
            pltpu.VMEM((1, instruments), jnp.float32),
            pltpu.VMEM((1, instruments), jnp.float32),
            pltpu.SMEM((K,), jnp.int32),
            pltpu.SemaphoreType.DMA((slots // 256,)),
            pltpu.SemaphoreType.DMA((instruments // 512,)),
            pltpu.SemaphoreType.DMA((4,)),
        ],
        compiler_params=pltpu.CompilerParams(vmem_limit_bytes=PRICE_VMEM),
        name="price",
    )


def body(axis, shocks, factor_sens, notional, moneyness, desk_entity, scenario_counts, candidate_ids):
    slots, factors = shocks.shape
    instruments = factor_sens.shape[1]
    cands = candidate_ids.shape[0]
    devices = lax.axis_size(axis)
    price = functools.partial(price_call, slots, factors, instruments, cands)
    args = (
        scenario_counts,
        desk_entity,
        candidate_ids.reshape(1, cands),
        notional.reshape(1, instruments),
        moneyness.reshape(1, instruments),
        shocks,
        factor_sens,
    )
    args = args[:1] + tuple(pltpu.with_memory_space_constraint(a, pltpu.HBM) for a in args[1:])
    sent = price(axis, devices)(*args)
    got = lax.all_to_all(sent, axis, 0, 0, tiled=True)
    tail, cand = pl.pallas_call(
        merge_kernel,
        out_shape=[
            jax.ShapeDtypeStruct((1, TOPK), jnp.float32),
            jax.ShapeDtypeStruct((cands // devices, ENT), jnp.float32),
        ],
        in_specs=[VMEM],
        out_specs=[VMEM, VMEM],
        compiler_params=pltpu.CompilerParams(vmem_limit_bytes=MERGE_VMEM),
        name="merge",
    )(got)
    return tail.reshape(TOPK), cand


def solution(mesh):
    return jax.shard_map(
        functools.partial(body, "scen"),
        mesh=mesh,
        in_specs=(P(("grp", "scen"), None), P(), P(), P(), P(), P(("grp", "scen")), P("grp")),
        out_specs=(P("grp"), P(("grp", "scen"), None)),
        check_vma=False,
    )
```

```python
import functools

import jax
import jax.numpy as jnp
from jax import lax
from jax.experimental import pallas as pl
from jax.experimental.pallas import tpu as pltpu
from jax.sharding import Mesh
from jax.sharding import PartitionSpec as P

K = 64
INSTR = 16
ENT = 8
TOPK = 256
LANES = 128
LOG2E = 1.4426950408889634
LN2 = 0.6931471805599453
LOW = -1e30
DELAY = 250

VMEM = pl.BlockSpec(memory_space=pltpu.VMEM)
SMEM = pl.BlockSpec(memory_space=pltpu.SMEM)
HBM = pl.BlockSpec(memory_space=pltpu.HBM)
PRICE_VMEM = 24 << 20
MERGE_VMEM = 8 << 20


def softplus2(t):
    return jnp.maximum(t, 0.0) + jnp.log2(1.0 + jnp.exp2(-jnp.abs(t)))


def iota(shape, dim):
    return lax.broadcasted_iota(jnp.int32, shape, dim)


def split_bf16(x):
    hi = x.astype(jnp.bfloat16)
    return hi, (x - hi.astype(jnp.float32)).astype(jnp.bfloat16)


def price_kernel(
    axes, devices, count_ref, desk_hbm, ids_hbm, notional_hbm, money_hbm, shocks_hbm, sens_hbm,
    out_ref, rows_ref, sens_ref, ent_w, res_ref, pick_ref, idc_ref, halves_ref, ids_ref, notional_ref,
    money_ref, base_ref, desk_ref, row_sems, sens_sems, small_sems,
):
    slots, factors = rows_ref.shape
    instruments = sens_ref.shape[1]
    cands = ids_ref.shape[1]
    step = 256
    blocks = slots // step
    pairs = instruments // (2 * step)
    deep = factors // step
    ch = 64
    chunks = step // ch
    mxus = (0, 1)

    half = factors // 2

    def row_copy(i):
        part = pl.ds(i * step, step)
        return pltpu.make_async_copy(shocks_hbm.at[part], rows_ref.at[part], row_sems.at[i])

    def first_copy(q):
        part = (pl.ds(0, step), pl.ds(q * half, half))
        return pltpu.make_async_copy(shocks_hbm.at[part], rows_ref.at[part], row_sems.at[blocks * q])

    def sens_copy(p, q):
        part = (pl.ds(q * half, half), pl.ds(p * 2 * step, 2 * step))
        return pltpu.make_async_copy(sens_hbm.at[part], sens_ref.at[part], sens_sems.at[p, q])

    small = [
        pltpu.make_async_copy(a, b, small_sems.at[n])
        for n, (a, b) in enumerate(
            (
                (desk_hbm, desk_ref),
                (ids_hbm, ids_ref),
                (notional_hbm, notional_ref),
                (money_hbm, money_ref),
            )
        )
    ]
    for copy in small:
        copy.start()
    first_copy(0).start()
    sens_copy(0, 0).start()
    pl.delay(DELAY)
    first_copy(1).start()
    sens_copy(0, 1).start()
    for copy in small:
        copy.wait()
    for p in range(1, pairs):
        for q in range(2):
            sens_copy(p, q).start()

    me = lax.axis_index(axes[0]) * lax.axis_size(axes[1]) + lax.axis_index(axes[1])
    lane = iota((INSTR, LANES), 1)
    for k in range(K):
        hit = (lane & (ENT - 1)) == desk_ref[k]
        ent_w[pl.ds(k * INSTR, INSTR), 0:LANES] = jnp.where(hit, -1.0, 0.0).astype(jnp.bfloat16)
    ent_w[:, LANES:] = jnp.full((instruments, LANES), -1.0, jnp.bfloat16)
    money_ref[...] = money_ref[...] * LOG2E
    base_ref[...] = softplus2(money_ref[...])
    notional_ref[...] = notional_ref[...] * LN2
    local = (ids_ref[...] - me * slots).astype(jnp.float32)
    for b in range(cands // LANES):
        span = pl.ds(b * LANES, LANES)
        row = jnp.broadcast_to(local[:, b * LANES : (b + 1) * LANES], (LANES, LANES))
        idc_ref[span, :] = jnp.transpose(row)

    spot = iota((step, LANES), 1).astype(jnp.float32)
    for i in range(cands // step):
        mine = slice(i * step, (i + 1) * step)
        for b in range(slots // LANES):
            hit = idc_ref[mine, :] == spot + float(b * LANES)
            pick_ref[mine, b * LANES : (b + 1) * LANES] = jnp.where(hit, 1.0, 0.0).astype(jnp.bfloat16)

    def main(accs):
        acc = {(q, m, c): accs[m][q * chunks + c] for q in mxus for m in mxus for c in range(chunks)}
        ent = {(m, c): accs[m][2 * chunks + c] for m in mxus for c in range(chunks)}

        def matmul(r, p, k):
            deep_k = slice(k * step, (k + 1) * step)
            for m in mxus:
                cols = slice((2 * p + m) * step, (2 * p + m + 1) * step)
                pltpu.matmul_push_rhs(sens_ref[deep_k, cols], 0, m)
            for c in range(chunks):
                at = pl.ds(r * step + c * ch, ch)
                lhs = rows_ref[at, deep_k]
                for m in mxus:
                    pltpu.matmul_acc_lhs(acc[p, m, c], lhs, 0 if c == 0 else None)

        def epilogue(p, m, c):
            cols = slice((2 * p + m) * step, (2 * p + m + 1) * step)
            value = pltpu.matmul_pop(acc[p, m, c])
            inst = notional_ref[:, cols] * (
                softplus2(value * LOG2E + money_ref[:, cols]) - base_ref[:, cols]
            )
            hi, lo = split_bf16(inst)
            halves_ref[m, 0, c * ch : (c + 1) * ch, :] = hi
            halves_ref[m, 1, c * ch : (c + 1) * ch, :] = lo

        def entities(p):
            for m in mxus:
                cols = slice((2 * p + m) * step, (2 * p + m + 1) * step)
                pltpu.matmul_push_rhs(ent_w[cols, :], 1, m)
            for h in range(2):
                for c in range(chunks):
                    for m in mxus:
                        part = halves_ref[m, h, c * ch : (c + 1) * ch, :]
                        pltpu.matmul_acc_lhs(ent[m, c], part, 1 if h + c == 0 else None)

        def collect(r):
            for c in range(chunks):
                at = pl.ds(r * step + c * ch, ch)
                res_ref[at, :] = pltpu.matmul_pop(ent[0, c]) + pltpu.matmul_pop(ent[1, c])

        def unit(r, p):
            last = 1 - p
            for k in range(deep):
                if r == 0 and k % (deep // 2) == 0:
                    q = k // (deep // 2)
                    if p == 0:
                        first_copy(q).wait()
                    sens_copy(p, q).wait()
                    if p + q == 0:
                        for i in range(1, blocks):
                            row_copy(i).start()
                matmul(r, p, k)
                if k % 2 == 1 and k // 2 < chunks and r + p > 0:
                    for m in mxus:
                        epilogue(last, m, k // 2)
                if p == 1 and k == 1 and r > 0:
                    collect(r - 1)
            if r + p > 0:
                entities(last)

        def one_block(r):
            if r == 1:
                for i in range(1, blocks):
                    row_copy(i).wait()
            unit(r, 0)
            unit(r, 1)

        for r in range(blocks):
            one_block(r)
        for c in range(chunks):
            for m in mxus:
                epilogue(1, m, c)
        entities(1)
        collect(blocks - 1)

        per = cands // devices
        keep = iota((1, per, LANES), 2) // ENT == iota((1, per, LANES), 1)
        for k in range(slots // step):
            hi, lo = split_bf16(res_ref[k * step : (k + 1) * step, 0:LANES])
            both = jnp.concatenate([hi, lo], axis=1)
            for m in mxus:
                pltpu.matmul_push_rhs(both, k % 2, m)
            for c in range(2 * chunks):
                for m in mxus:
                    at = m * (cands // 2) + c * ch
                    lhs = pick_ref[at : at + ch, k * step : (k + 1) * step]
                    pltpu.matmul_acc_lhs(accs[m][c], lhs, k % 2 if c == 0 else None)

        groups = slots // LANES
        count = count_ref[0]
        col = jnp.where(iota((slots, LANES), 0) < count, res_ref[:, LANES:], LOW)
        eye = iota((LANES, LANES), 0) == iota((LANES, LANES), 1)
        before = iota((LANES, LANES), 1) < iota((LANES, LANES), 0)
        rows = []
        for b in range(groups):
            here = col[b * LANES : (b + 1) * LANES]
            row = jnp.sum(jnp.where(eye, here, 0.0), axis=0, keepdims=True)
            rows.append(jnp.broadcast_to(row, (LANES, LANES)))
        ones = jnp.ones((step, step), jnp.bfloat16)
        for m in mxus:
            pltpu.matmul_push_rhs(ones, 0, m)
        for a in range(groups):
            mine = col[a * LANES : (a + 1) * LANES]
            sums = []
            for half in range(2):
                acc_a = jnp.zeros((LANES, LANES), jnp.float32)
                for b in range(half * groups // 2, (half + 1) * groups // 2):
                    row = rows[b]
                    if b < a:
                        ahead = row >= mine
                    elif b > a:
                        ahead = row > mine
                    else:
                        ahead = (row > mine) | ((row == mine) & before)
                    acc_a = acc_a + jnp.where(ahead, 1.0, 0.0)
                sums.append(acc_a.astype(jnp.bfloat16))
            both = jnp.concatenate(sums, axis=1)
            m, a_m = a % 2, a // 2
            for c in range(2):
                pltpu.matmul_acc_lhs(
                    accs[m][2 * chunks + 2 * a_m + c],
                    both[c * ch : (c + 1) * ch],
                    0 if a_m + c == 0 else None,
                )
        for m in mxus:
            for c in range(2 * chunks):
                got = pltpu.matmul_pop(accs[m][c])
                got = (got[:, 0:LANES] + got[:, LANES:]).reshape(ch // per, per, LANES)
                at = (m * (cands // 2) + c * ch) // per
                out_ref[at : at + ch // per, :, TOPK:] = jnp.sum(
                    jnp.where(keep, got, 0.0), axis=1, keepdims=True
                )
        rising = lax.axis_index(axes[0]) >= devices // 2
        lines = [jnp.zeros((ch, LANES), jnp.float32) for _ in range(TOPK // LANES)]
        spots = []
        for h in range(TOPK // LANES):
            place = iota((ch, LANES), 1) + h * LANES
            spots.append(jnp.where(rising, TOPK - 1 - place, place).astype(jnp.float32))
        for a in range(groups):
            for c in range(2):
                rank = pltpu.matmul_pop(accs[a % 2][2 * chunks + 2 * (a // 2) + c])[:, 0:LANES]
                at = a * LANES + c * ch
                for h in range(TOPK // LANES):
                    lines[h] = lines[h] + jnp.where(rank == spots[h], col[at : at + ch], 0.0)
        for h in range(TOPK // LANES):
            line = jnp.sum(lines[h], axis=0, keepdims=True)
            out_ref[:, :, h * LANES : (h + 1) * LANES] = jnp.broadcast_to(
                line[None], (devices, 1, LANES)
            )

    accs = [[pltpu.ACC(m)((ch, step), jnp.float32) for _ in range(4 * chunks)] for m in mxus]
    pl.run_scoped(lambda *refs: main((refs[: 4 * chunks], refs[4 * chunks :])), *accs[0], *accs[1])


def merge_kernel(in_ref, own_ref, send_ref):
    devices = in_ref.shape[0]
    lists = in_ref[...].reshape(devices, in_ref.shape[2])
    sums = jnp.sum(lists[:, TOPK:], axis=0, keepdims=True)
    own_ref[:, TOPK:] = sums
    send_ref[:, TOPK:] = sums

    lists = jnp.concatenate([lists[:, 0:TOPK]] * (LANES // devices), axis=0)
    turned = [jnp.transpose(lists[:, h * LANES : (h + 1) * LANES]) for h in range(TOPK // LANES)]
    per = LANES // 8
    x = [turned[g // per][8 * (g % per) : 8 * (g % per) + 8] for g in range(TOPK // 8)]
    lane = iota((8, LANES), 1)
    sub = iota((8, LANES), 0)

    def ordered(x):
        gap = len(x) // 2
        while gap:
            new = list(x)
            for g in range(len(x)):
                if not g & gap:
                    new[g] = jnp.maximum(x[g], x[g + gap])
                    new[g + gap] = jnp.minimum(x[g], x[g + gap])
            x, gap = new, gap // 2
        for gap in (4, 2, 1):
            upper = (sub & gap) == 0
            new = []
            for v in x:
                other = pltpu.roll(v, 8 - gap, 0)
                low = pltpu.roll(jnp.minimum(v, other), gap, 0)
                new.append(jnp.where(upper, jnp.maximum(v, other), low))
            x = new
        return x

    gap = devices // 2
    while gap:
        x = [jnp.maximum(v, pltpu.roll(v, gap, 1)) for v in x]
        gap //= 2
        if gap:
            sign = jnp.where((lane & gap) == 0, 1.0, -1.0)
            x = [v * sign for v in ordered([v * sign for v in x])]
    x = ordered(x)
    for h in range(TOPK // LANES):
        fall = rise = jnp.zeros((8, LANES), jnp.float32)
        for g in range(per):
            v = x[h * per + g]
            fall = fall + jnp.where(lane == sub + 8 * g, v, 0.0)
            rise = rise + jnp.where(lane == LANES - 1 - sub - 8 * g, v, 0.0)
        own_ref[:, h * LANES : (h + 1) * LANES] = jnp.sum(fall, axis=0, keepdims=True)
        other = TOPK - (h + 1) * LANES
        send_ref[:, other : other + LANES] = jnp.sum(rise, axis=0, keepdims=True)


def join_kernel(core_axis, own_ref, came_ref, tail_ref, cand_ref):
    total = own_ref[:, TOPK:] + came_ref[:, TOPK:]
    per = LANES // lax.axis_size(core_axis)
    total = jnp.where(lax.axis_index(core_axis) == 0, total, pltpu.roll(total, per, 1))
    spread = jnp.where(iota((8, LANES), 1) // ENT == iota((8, LANES), 0), total, 0.0)
    for d in (32, 16, 8):
        spread = spread + pltpu.roll(spread, LANES - d, 1)
    cand_ref[...] = spread[:, 0:ENT]

    parts = range(TOPK // LANES)
    rows = []
    cols = []
    for h in parts:
        span = slice(h * LANES, (h + 1) * LANES)
        rows.append(jnp.broadcast_to(jnp.maximum(own_ref[:, span], came_ref[:, span]), (LANES, LANES)))
        cols.append(jnp.transpose(rows[h]))
    before = iota((LANES, LANES), 1) < iota((LANES, LANES), 0)
    lines = [jnp.zeros((1, LANES), jnp.float32) for _ in parts]
    for a in parts:
        ahead = jnp.zeros((LANES, LANES), jnp.float32)
        for b in parts:
            if b < a:
                first = rows[b] >= cols[a]
            elif b > a:
                first = rows[b] > cols[a]
            else:
                first = (rows[b] > cols[a]) | ((rows[b] == cols[a]) & before)
            ahead = ahead + jnp.where(first, 1.0, 0.0)
        rank = jnp.sum(ahead, axis=1, keepdims=True)
        for h in parts:
            place = (iota((LANES, LANES), 1) + h * LANES).astype(jnp.float32)
            picked = jnp.where(rank == place, cols[a], 0.0)
            lines[h] = lines[h] + jnp.sum(picked, axis=0, keepdims=True)
    for h in parts:
        tail_ref[:, h * LANES : (h + 1) * LANES] = lines[h]


def price_call(slots, factors, instruments, cands, axes, devices):
    return pl.pallas_call(
        functools.partial(price_kernel, axes, devices),
        out_shape=jax.ShapeDtypeStruct((devices, 1, TOPK + LANES), jnp.float32),
        in_specs=[SMEM] + [HBM] * 6,
        out_specs=VMEM,
        scratch_shapes=[
            pltpu.VMEM((slots, factors), jnp.bfloat16),
            pltpu.VMEM((factors, instruments), jnp.bfloat16),
            pltpu.VMEM((instruments, 2 * LANES), jnp.bfloat16),
            pltpu.VMEM((slots, 2 * LANES), jnp.float32),
            pltpu.VMEM((cands, slots), jnp.bfloat16),
            pltpu.VMEM((cands, LANES), jnp.float32),
            pltpu.VMEM((2, 2, 256, 256), jnp.bfloat16),
            pltpu.VMEM((1, cands), jnp.int32),
            pltpu.VMEM((1, instruments), jnp.float32),
            pltpu.VMEM((1, instruments), jnp.float32),
            pltpu.VMEM((1, instruments), jnp.float32),
            pltpu.SMEM((K,), jnp.int32),
            pltpu.SemaphoreType.DMA((slots // 256 + 1,)),
            pltpu.SemaphoreType.DMA((instruments // 512, 2)),
            pltpu.SemaphoreType.DMA((4,)),
        ],
        compiler_params=pltpu.CompilerParams(vmem_limit_bytes=PRICE_VMEM),
        name="price",
    )


def body(shocks, factor_sens, notional, moneyness, desk_entity, scenario_counts, candidate_ids):
    slots, factors = shocks.shape
    instruments = factor_sens.shape[1]
    cands = candidate_ids.shape[0]
    chips, cores = lax.axis_size("chip"), lax.axis_size("core")
    args = (
        scenario_counts,
        desk_entity,
        candidate_ids.reshape(1, cands),
        notional.reshape(1, instruments),
        moneyness.reshape(1, instruments),
        shocks,
        factor_sens,
    )
    args = args[:1] + tuple(pltpu.with_memory_space_constraint(a, pltpu.HBM) for a in args[1:])
    price = price_call(slots, factors, instruments, cands, ("chip", "core"), chips)
    got = lax.all_to_all(price(*args), "chip", 0, 0, tiled=True)
    line = jax.ShapeDtypeStruct((1, TOPK + LANES), jnp.float32)
    own, send = pl.pallas_call(
        merge_kernel,
        out_shape=[line, line],
        in_specs=[VMEM],
        out_specs=[VMEM, VMEM],
        compiler_params=pltpu.CompilerParams(vmem_limit_bytes=MERGE_VMEM),
        name="merge",
    )(got)
    came = lax.ppermute(send, "core", [(0, 1), (1, 0)])
    tail, cand = pl.pallas_call(
        functools.partial(join_kernel, "core"),
        out_shape=[
            jax.ShapeDtypeStruct((1, TOPK), jnp.float32),
            jax.ShapeDtypeStruct((cands // (chips * cores), ENT), jnp.float32),
        ],
        in_specs=[VMEM, VMEM],
        out_specs=[VMEM, VMEM],
        compiler_params=pltpu.CompilerParams(vmem_limit_bytes=MERGE_VMEM),
        name="join",
    )(own, came)
    return tail.reshape(TOPK), cand


def solution(mesh):
    groups, scen = mesh.shape["grp"], mesh.shape["scen"]
    finer = Mesh(mesh.devices.reshape(groups, scen // 2, 2), ("grp", "chip", "core"))
    every = ("grp", "chip", "core")
    return jax.shard_map(
        body,
        mesh=finer,
        in_specs=(P(every, None), P(), P(), P(), P(), P(every), P("grp")),
        out_specs=(P("grp"), P(every, None)),
        check_vma=False,
    )
```

```python
import functools

import jax
import jax.numpy as jnp
from jax import lax
from jax.experimental import pallas as pl
from jax.experimental.pallas import tpu as pltpu
from jax.sharding import Mesh
from jax.sharding import PartitionSpec as P

K = 64
INSTR = 16
ENT = 8
TOPK = 256
LANES = 128
LOG2E = 1.4426950408889634
LN2 = 0.6931471805599453
LOW = -1e30
DELAY = 250

VMEM = pl.BlockSpec(memory_space=pltpu.VMEM)
SMEM = pl.BlockSpec(memory_space=pltpu.SMEM)
HBM = pl.BlockSpec(memory_space=pltpu.HBM)
PRICE_VMEM = 24 << 20
MERGE_VMEM = 8 << 20


def softplus2(t):
    return jnp.maximum(t, 0.0) + jnp.log2(1.0 + jnp.exp2(-jnp.abs(t)))


def iota(shape, dim):
    return lax.broadcasted_iota(jnp.int32, shape, dim)


def split_bf16(x):
    hi = x.astype(jnp.bfloat16)
    return hi, (x - hi.astype(jnp.float32)).astype(jnp.bfloat16)


def price_kernel(
    axes, devices, count_ref, desk_hbm, ids_hbm, notional_hbm, money_hbm, shocks_hbm, sens_hbm,
    out_ref, rows_ref, sens_ref, ent_w, res_ref, pick_ref, idc_ref, halves_ref, ids_ref, notional_ref,
    money_ref, base_ref, line_ref, best_ref, desk_ref, row_sems, sens_sems, small_sems,
):
    slots, factors = rows_ref.shape
    instruments = sens_ref.shape[1]
    cands = ids_ref.shape[1]
    step = 256
    blocks = slots // step
    pairs = instruments // (2 * step)
    deep = factors // step
    ch = 64
    chunks = step // ch
    mxus = (0, 1)

    half = factors // 2

    def row_copy(i):
        part = pl.ds(i * step, step)
        return pltpu.make_async_copy(shocks_hbm.at[part], rows_ref.at[part], row_sems.at[i])

    def first_copy(q):
        part = (pl.ds(0, step), pl.ds(q * half, half))
        return pltpu.make_async_copy(shocks_hbm.at[part], rows_ref.at[part], row_sems.at[blocks * q])

    def sens_copy(p, q):
        part = (pl.ds(q * half, half), pl.ds(p * 2 * step, 2 * step))
        return pltpu.make_async_copy(sens_hbm.at[part], sens_ref.at[part], sens_sems.at[p, q])

    small = [
        pltpu.make_async_copy(a, b, small_sems.at[n])
        for n, (a, b) in enumerate(
            (
                (desk_hbm, desk_ref),
                (ids_hbm, ids_ref),
                (notional_hbm, notional_ref),
                (money_hbm, money_ref),
            )
        )
    ]
    for copy in small:
        copy.start()
    first_copy(0).start()
    sens_copy(0, 0).start()
    pl.delay(DELAY)
    first_copy(1).start()
    sens_copy(0, 1).start()
    pl.delay(DELAY)
    for p in range(1, pairs):
        for q in range(2):
            sens_copy(p, q).start()
    me = lax.axis_index(axes[0]) * lax.axis_size(axes[1]) + lax.axis_index(axes[1])

    def tables():
        for copy in small:
            copy.wait()
        lane = iota((INSTR, LANES), 1)
        upper = iota((INSTR, LANES), 0) < INSTR // 2
        per_tile = LANES // INSTR
        for k in range(instruments // (2 * INSTR)):
            desk = k // per_tile * 2 * per_tile + k % per_tile
            entity = jnp.where(upper, desk_ref[desk], desk_ref[desk + per_tile])
            hit = (lane & (ENT - 1)) == entity
            ent_w[pl.ds(k * INSTR, INSTR), 0:LANES] = jnp.where(hit, -1.0, 0.0).astype(jnp.bfloat16)
        ent_w[:, LANES:] = jnp.full((instruments // 2, LANES), -1.0, jnp.bfloat16)
        money_ref[...] = money_ref[...] * LOG2E
        base_ref[...] = softplus2(money_ref[...])
        notional_ref[...] = notional_ref[...] * LN2
        local = (ids_ref[...] - me * slots).astype(jnp.float32)
        for b in range(cands // LANES):
            span = pl.ds(b * LANES, LANES)
            row = jnp.broadcast_to(local[:, b * LANES : (b + 1) * LANES], (LANES, LANES))
            idc_ref[span, :] = jnp.transpose(row)

    spot = iota((step, LANES), 1).astype(jnp.float32)
    def picks(i):
        mine = slice(i * step, (i + 1) * step)
        for b in range(slots // LANES):
            hit = idc_ref[mine, :] == spot + float(b * LANES)
            pick_ref[mine, b * LANES : (b + 1) * LANES] = jnp.where(hit, 1.0, 0.0).astype(jnp.bfloat16)

    def main(accs):
        acc = {(q, m, c): accs[m][q * chunks + c] for q in mxus for m in mxus for c in range(chunks)}
        ent = {(m, c): accs[m][2 * chunks + c] for m in mxus for c in range(chunks)}

        def matmul(r, p, k):
            deep_k = slice(k * step, (k + 1) * step)
            for m in mxus:
                cols = slice((2 * p + m) * step, (2 * p + m + 1) * step)
                pltpu.matmul_push_rhs(sens_ref[deep_k, cols], 0, m)
            for c in range(chunks):
                at = pl.ds(r * step + c * ch, ch)
                lhs = rows_ref[at, deep_k]
                for m in mxus:
                    pltpu.matmul_acc_lhs(acc[p, m, c], lhs, 0 if c == 0 else None)

        left = (iota((ch, LANES), 1) & (INSTR - 1)) < INSTR // 2

        def epilogue(p, c):
            tiles = []
            for m in mxus:
                cols = slice((2 * p + m) * step, (2 * p + m + 1) * step)
                value = pltpu.matmul_pop(acc[p, m, c])
                inst = notional_ref[:, cols] * (
                    softplus2(value * LOG2E + money_ref[:, cols]) - base_ref[:, cols]
                )
                a, b = inst[:, 0:LANES], inst[:, LANES:]
                a = a + pltpu.roll(a, LANES - INSTR // 2, 1)
                b = b + pltpu.roll(b, INSTR // 2, 1)
                tiles.append(jnp.where(left, a, b))
            hi, lo = split_bf16(jnp.concatenate(tiles, axis=1))
            halves_ref[0, c * ch : (c + 1) * ch, :] = hi
            halves_ref[1, c * ch : (c + 1) * ch, :] = lo

        def entities(p):
            for m in mxus:
                pltpu.matmul_push_rhs(ent_w[p * step : (p + 1) * step, :], 1, m)
            for c in range(chunks):
                for m in mxus:
                    part = halves_ref[m, c * ch : (c + 1) * ch, :]
                    pltpu.matmul_acc_lhs(ent[m, c], part, 1 if c == 0 else None)

        def collect(r):
            for c in range(chunks):
                at = pl.ds(r * step + c * ch, ch)
                sums = pltpu.matmul_pop(ent[0, c]) + pltpu.matmul_pop(ent[1, c])
                res_ref[at, 0:LANES] = sums[:, 0:LANES]
                valid = iota((ch, LANES), 0) + (r * step + c * ch) < count
                res_ref[at, LANES:] = jnp.where(valid, sums[:, LANES:], LOW)

        count = count_ref[0]
        lane8 = iota((8, LANES), 1)
        sub = iota((8, LANES), 0)
        lists = TOPK // LANES
        per8 = LANES // 8

        def as_row(col):
            line = jnp.zeros((8, LANES), jnp.float32)
            for g in range(per8):
                line = line + jnp.where(lane8 == sub + 8 * g, col(8 * g), 0.0)
            return jnp.broadcast_to(jnp.sum(line, axis=0, keepdims=True), (8, LANES))

        def losses(block):
            return lambda at: res_ref[block * LANES + at : block * LANES + at + 8, LANES:]

        def join(r, places):
            cols = [
                losses(q) if r == 1 else (lambda at, q=q: best_ref[q * LANES + at : q * LANES + at + 8, :])
                for q in range(lists)
            ]
            fresh = step // LANES
            cols += [losses(r * fresh + q) for q in range(fresh)]
            for b in range(0 if r == 1 else lists, lists + fresh):
                line_ref[8 * b : 8 * b + 8, :] = as_row(cols[b])
            out = [jnp.zeros((8, LANES), jnp.float32) for _ in range(lists)]
            for a in range(lists + fresh):
                known = a < lists and r > 1
                for g in range(per8):
                    col = cols[a](8 * g)
                    ahead = jnp.zeros((8, LANES), jnp.float32)
                    for b in range(lists if known else 0, lists + fresh):
                        row = line_ref[8 * b : 8 * b + 8, :]
                        if b < a:
                            first = row >= col
                        elif b > a:
                            first = row > col
                        else:
                            first = (row > col) | ((row == col) & (lane8 < sub + 8 * g))
                        ahead = ahead + jnp.where(first, 1.0, 0.0)
                    rank = jnp.broadcast_to(jnp.sum(ahead, axis=1, keepdims=True), (8, LANES))
                    if known:
                        rank = rank + (sub + (a * LANES + 8 * g)).astype(jnp.float32)
                    for h in range(lists):
                        out[h] = out[h] + jnp.where(rank == places[h], col, 0.0)
            return [jnp.sum(out[h], axis=0, keepdims=True) for h in range(lists)]

        upright = [(lane8 + h * LANES).astype(jnp.float32) for h in range(lists)]

        def compare(r):
            if r == 0:
                return
            for h, line in enumerate(join(r, upright)):
                line_ref[8 * h : 8 * h + 8, :] = jnp.broadcast_to(line, (8, LANES))
                best_ref[h * LANES : (h + 1) * LANES, :] = jnp.transpose(
                    jnp.broadcast_to(line, (LANES, LANES))
                )

        def unit(r, p):
            last = 1 - p
            for k in range(deep):
                if r == 0 and k % (deep // 2) == 0:
                    q = k // (deep // 2)
                    if p == 0:
                        first_copy(q).wait()
                    sens_copy(p, q).wait()
                    if p == 0 and q == 1:
                        row_copy(1).start()
                    if p == 1 and q == 0:
                        for i in range(2, blocks):
                            row_copy(i).start()
                matmul(r, p, k)
                if r + p == 0 and k == 0:
                    tables()
                if r + p == 0 and k % 2 == 1:
                    picks(k // 2)
                if k % 2 == 1 and k // 2 < chunks and r + p > 0:
                    epilogue(last, k // 2)
                if p == 1 and k == 1 and r > 0:
                    collect(r - 1)
                    compare(r - 1)
            if r + p > 0:
                entities(last)

        def one_block(r):
            if r == 1:
                row_copy(1).wait()
            if r == 2:
                for i in range(2, blocks):
                    row_copy(i).wait()
            unit(r, 0)
            unit(r, 1)

        for r in range(blocks):
            one_block(r)
        cand_accs = [accs[m][:chunks] + accs[m][3 * chunks :] for m in mxus]

        def route(k):
            hi, lo = split_bf16(res_ref[k * step : (k + 1) * step, 0:LANES])
            both = jnp.concatenate([hi, lo], axis=1)
            for m in mxus:
                pltpu.matmul_push_rhs(both, 0, m)
            for c in range(2 * chunks):
                for m in mxus:
                    at = m * (cands // 2) + c * ch
                    lhs = pick_ref[at : at + ch, k * step : (k + 1) * step]
                    pltpu.matmul_acc_lhs(cand_accs[m][c], lhs, 0 if c == 0 else None)

        for k in range(0):
            route(k)
        for c in range(chunks):
            epilogue(1, c)
        entities(1)
        for k in range(0, blocks - 1):
            route(k)
        collect(blocks - 1)
        route(blocks - 1)
        flip = lax.axis_index(axes[0]) >= devices // 2
        places = [jnp.where(flip, TOPK - 1 - place, place) for place in upright]
        for h, line in enumerate(join(blocks - 1, places)):
            out_ref[:, :, h * LANES : (h + 1) * LANES] = jnp.broadcast_to(
                line[None], (devices, 1, LANES)
            )
        per = cands // devices
        keep = iota((1, per, LANES), 2) // ENT == iota((1, per, LANES), 1)
        for m in mxus:
            for c in range(2 * chunks):
                got = pltpu.matmul_pop(cand_accs[m][c])
                got = (got[:, 0:LANES] + got[:, LANES:]).reshape(ch // per, per, LANES)
                at = (m * (cands // 2) + c * ch) // per
                out_ref[at : at + ch // per, :, TOPK:] = jnp.sum(
                    jnp.where(keep, got, 0.0), axis=1, keepdims=True
                )

    accs = [[pltpu.ACC(m)((ch, step), jnp.float32) for _ in range(4 * chunks)] for m in mxus]
    pl.run_scoped(lambda *refs: main((refs[: 4 * chunks], refs[4 * chunks :])), *accs[0], *accs[1])


def merge_kernel(in_ref, own_ref, send_ref):
    devices = in_ref.shape[0]
    lists = in_ref[...].reshape(devices, in_ref.shape[2])
    sums = jnp.sum(lists[:, TOPK:], axis=0, keepdims=True)
    own_ref[:, TOPK:] = sums
    send_ref[:, TOPK:] = sums

    lists = jnp.concatenate([lists[:, 0:TOPK]] * (LANES // devices), axis=0)
    turned = [jnp.transpose(lists[:, h * LANES : (h + 1) * LANES]) for h in range(TOPK // LANES)]
    per = LANES // 8
    x = [turned[g // per][8 * (g % per) : 8 * (g % per) + 8] for g in range(TOPK // 8)]
    lane = iota((8, LANES), 1)
    sub = iota((8, LANES), 0)

    def ordered(x):
        gap = len(x) // 2
        while gap:
            new = list(x)
            for g in range(len(x)):
                if not g & gap:
                    new[g] = jnp.maximum(x[g], x[g + gap])
                    new[g + gap] = jnp.minimum(x[g], x[g + gap])
            x, gap = new, gap // 2
        for gap in (4, 2, 1):
            upper = (sub & gap) == 0
            new = []
            for v in x:
                other = pltpu.roll(v, 8 - gap, 0)
                low = pltpu.roll(jnp.minimum(v, other), gap, 0)
                new.append(jnp.where(upper, jnp.maximum(v, other), low))
            x = new
        return x

    gap = devices // 2
    while gap:
        x = [jnp.maximum(v, pltpu.roll(v, gap, 1)) for v in x]
        gap //= 2
        if gap:
            sign = jnp.where((lane & gap) == 0, 1.0, -1.0)
            x = [v * sign for v in ordered([v * sign for v in x])]
    x = ordered(x)
    for h in range(TOPK // LANES):
        fall = rise = jnp.zeros((8, LANES), jnp.float32)
        for g in range(per):
            v = x[h * per + g]
            fall = fall + jnp.where(lane == sub + 8 * g, v, 0.0)
            rise = rise + jnp.where(lane == LANES - 1 - sub - 8 * g, v, 0.0)
        own_ref[:, h * LANES : (h + 1) * LANES] = jnp.sum(fall, axis=0, keepdims=True)
        other = TOPK - (h + 1) * LANES
        send_ref[:, other : other + LANES] = jnp.sum(rise, axis=0, keepdims=True)


def join_kernel(core_axis, own_ref, came_ref, tail_ref, cand_ref):
    total = own_ref[:, TOPK:] + came_ref[:, TOPK:]
    per = LANES // lax.axis_size(core_axis)
    total = jnp.where(lax.axis_index(core_axis) == 0, total, pltpu.roll(total, per, 1))
    spread = jnp.where(iota((8, LANES), 1) // ENT == iota((8, LANES), 0), total, 0.0)
    for d in (32, 16, 8):
        spread = spread + pltpu.roll(spread, LANES - d, 1)
    cand_ref[...] = spread[:, 0:ENT]

    parts = range(TOPK // LANES)
    rows = []
    cols = []
    for h in parts:
        span = slice(h * LANES, (h + 1) * LANES)
        rows.append(jnp.broadcast_to(jnp.maximum(own_ref[:, span], came_ref[:, span]), (LANES, LANES)))
        cols.append(jnp.transpose(rows[h]))
    before = iota((LANES, LANES), 1) < iota((LANES, LANES), 0)
    lines = [jnp.zeros((1, LANES), jnp.float32) for _ in parts]
    for a in parts:
        ahead = jnp.zeros((LANES, LANES), jnp.float32)
        for b in parts:
            if b < a:
                first = rows[b] >= cols[a]
            elif b > a:
                first = rows[b] > cols[a]
            else:
                first = (rows[b] > cols[a]) | ((rows[b] == cols[a]) & before)
            ahead = ahead + jnp.where(first, 1.0, 0.0)
        rank = jnp.sum(ahead, axis=1, keepdims=True)
        for h in parts:
            place = (iota((LANES, LANES), 1) + h * LANES).astype(jnp.float32)
            picked = jnp.where(rank == place, cols[a], 0.0)
            lines[h] = lines[h] + jnp.sum(picked, axis=0, keepdims=True)
    for h in parts:
        tail_ref[:, h * LANES : (h + 1) * LANES] = lines[h]


def price_call(slots, factors, instruments, cands, axes, devices):
    return pl.pallas_call(
        functools.partial(price_kernel, axes, devices),
        out_shape=jax.ShapeDtypeStruct((devices, 1, TOPK + LANES), jnp.float32),
        in_specs=[SMEM] + [HBM] * 6,
        out_specs=VMEM,
        scratch_shapes=[
            pltpu.VMEM((slots, factors), jnp.bfloat16),
            pltpu.VMEM((factors, instruments), jnp.bfloat16),
            pltpu.VMEM((instruments // 2, 2 * LANES), jnp.bfloat16),
            pltpu.VMEM((slots, 2 * LANES), jnp.float32),
            pltpu.VMEM((cands, slots), jnp.bfloat16),
            pltpu.VMEM((cands, LANES), jnp.float32),
            pltpu.VMEM((2, 256, 256), jnp.bfloat16),
            pltpu.VMEM((1, cands), jnp.int32),
            pltpu.VMEM((1, instruments), jnp.float32),
            pltpu.VMEM((1, instruments), jnp.float32),
            pltpu.VMEM((1, instruments), jnp.float32),
            pltpu.VMEM((32, LANES), jnp.float32),
            pltpu.VMEM((TOPK, LANES), jnp.float32),
            pltpu.SMEM((K,), jnp.int32),
            pltpu.SemaphoreType.DMA((slots // 256 + 1,)),
            pltpu.SemaphoreType.DMA((instruments // 512, 2)),
            pltpu.SemaphoreType.DMA((4,)),
        ],
        compiler_params=pltpu.CompilerParams(vmem_limit_bytes=PRICE_VMEM),
        name="price",
    )


def body(shocks, factor_sens, notional, moneyness, desk_entity, scenario_counts, candidate_ids):
    slots, factors = shocks.shape
    instruments = factor_sens.shape[1]
    cands = candidate_ids.shape[0]
    chips, cores = lax.axis_size("chip"), lax.axis_size("core")
    args = (
        scenario_counts,
        desk_entity,
        candidate_ids.reshape(1, cands),
        notional.reshape(1, instruments),
        moneyness.reshape(1, instruments),
        shocks,
        factor_sens,
    )
    args = args[:1] + tuple(pltpu.with_memory_space_constraint(a, pltpu.HBM) for a in args[1:])
    price = price_call(slots, factors, instruments, cands, ("chip", "core"), chips)
    got = lax.all_to_all(price(*args), "chip", 0, 0, tiled=True)
    line = jax.ShapeDtypeStruct((1, TOPK + LANES), jnp.float32)
    own, send = pl.pallas_call(
        merge_kernel,
        out_shape=[line, line],
        in_specs=[VMEM],
        out_specs=[VMEM, VMEM],
        compiler_params=pltpu.CompilerParams(vmem_limit_bytes=MERGE_VMEM),
        name="merge",
    )(got)
    came = lax.ppermute(send, "core", [(0, 1), (1, 0)])
    tail, cand = pl.pallas_call(
        functools.partial(join_kernel, "core"),
        out_shape=[
            jax.ShapeDtypeStruct((1, TOPK), jnp.float32),
            jax.ShapeDtypeStruct((cands // (chips * cores), ENT), jnp.float32),
        ],
        in_specs=[VMEM, VMEM],
        out_specs=[VMEM, VMEM],
        compiler_params=pltpu.CompilerParams(vmem_limit_bytes=MERGE_VMEM),
        name="join",
    )(own, came)
    return tail.reshape(TOPK), cand


def solution(mesh):
    groups, scen = mesh.shape["grp"], mesh.shape["scen"]
    finer = Mesh(mesh.devices.reshape(groups, scen // 2, 2), ("grp", "chip", "core"))
    every = ("grp", "chip", "core")
    return jax.shard_map(
        body,
        mesh=finer,
        in_specs=(P(every, None), P(), P(), P(), P(), P(every), P("grp")),
        out_specs=(P("grp"), P(every, None)),
        check_vma=False,
    )
```

```python
import functools

import jax
import jax.numpy as jnp
from jax import lax
from jax.experimental import pallas as pl
from jax.experimental.pallas import tpu as pltpu
from jax.sharding import Mesh
from jax.sharding import PartitionSpec as P

K = 64
INSTR = 16
ENT = 8
TOPK = 256
LANES = 128
LOG2E = 1.4426950408889634
LN2 = 0.6931471805599453
LOW = -1e30
DELAY = 250

VMEM = pl.BlockSpec(memory_space=pltpu.VMEM)
SMEM = pl.BlockSpec(memory_space=pltpu.SMEM)
HBM = pl.BlockSpec(memory_space=pltpu.HBM)
PRICE_VMEM = 24 << 20
MERGE_VMEM = 8 << 20


def softplus2(t):
    return jnp.maximum(t, 0.0) + jnp.log2(1.0 + jnp.exp2(-jnp.abs(t)))


def iota(shape, dim):
    return lax.broadcasted_iota(jnp.int32, shape, dim)


def split_bf16(x):
    hi = x.astype(jnp.bfloat16)
    return hi, (x - hi.astype(jnp.float32)).astype(jnp.bfloat16)


def price_kernel(
    axes, devices, count_ref, desk_hbm, ids_hbm, notional_hbm, money_hbm, shocks_hbm, sens_hbm,
    out_ref, ent_w, res_ref, pick_ref, idc_ref, halves_ref, ids_ref, notional_ref,
    money_ref, base_ref, line_ref, best_ref, desk_ref, row_sems, sens_sems, small_sems,
):
    def whole(rows_ref, sens_ref):
        slots, factors = shocks_hbm.shape
        instruments = sens_hbm.shape[1]
        cands = ids_ref.shape[1]
        step = 256
        blocks = slots // step
        pairs = instruments // (2 * step)
        deep = factors // step
        ch = 64
        chunks = step // ch
        mxus = (0, 1)

        half = factors // 2

        def row_copy(i):
            part = pl.ds(i * step, step)
            return pltpu.make_async_copy(shocks_hbm.at[part], rows_ref.at[part], row_sems.at[i])

        def first_copy(q):
            part = (pl.ds(0, step), pl.ds(q * half, half))
            return pltpu.make_async_copy(shocks_hbm.at[part], rows_ref.at[part], row_sems.at[blocks * q])

        def sens_copy(p, q):
            part = (pl.ds(q * half, half), pl.ds(p * 2 * step, 2 * step))
            return pltpu.make_async_copy(sens_hbm.at[part], sens_ref.at[part], sens_sems.at[p, q])

        small = [
            pltpu.make_async_copy(a, b, small_sems.at[n])
            for n, (a, b) in enumerate(
                (
                    (desk_hbm, desk_ref),
                    (ids_hbm, ids_ref),
                    (notional_hbm, notional_ref),
                    (money_hbm, money_ref),
                )
            )
        ]
        for copy in small:
            copy.start()
        first_copy(0).start()
        sens_copy(0, 0).start()
        pl.delay(DELAY)
        first_copy(1).start()
        sens_copy(0, 1).start()
        pl.delay(DELAY)
        for p in range(1, pairs):
            for q in range(2):
                sens_copy(p, q).start()
        me = lax.axis_index(axes[0]) * lax.axis_size(axes[1]) + lax.axis_index(axes[1])

        def tables():
            for copy in small:
                copy.wait()
            lane = iota((INSTR, LANES), 1)
            upper = iota((INSTR, LANES), 0) < INSTR // 2
            per_tile = LANES // INSTR
            for k in range(instruments // (2 * INSTR)):
                desk = k // per_tile * 2 * per_tile + k % per_tile
                entity = jnp.where(upper, desk_ref[desk], desk_ref[desk + per_tile])
                hit = (lane & (ENT - 1)) == entity
                ent_w[pl.ds(k * INSTR, INSTR), 0:LANES] = jnp.where(hit, -1.0, 0.0).astype(jnp.bfloat16)
            ent_w[:, LANES:] = jnp.full((instruments // 2, LANES), -1.0, jnp.bfloat16)
            money_ref[...] = money_ref[...] * LOG2E
            base_ref[...] = softplus2(money_ref[...])
            notional_ref[...] = notional_ref[...] * LN2
            local = (ids_ref[...] - me * slots).astype(jnp.float32)
            for b in range(cands // LANES):
                span = pl.ds(b * LANES, LANES)
                row = jnp.broadcast_to(local[:, b * LANES : (b + 1) * LANES], (LANES, LANES))
                idc_ref[span, :] = jnp.transpose(row)

        spot = iota((step, LANES), 1).astype(jnp.float32)
        def picks(i):
            mine = slice(i * step, (i + 1) * step)
            for b in range(slots // LANES):
                hit = idc_ref[mine, :] == spot + float(b * LANES)
                pick_ref[mine, b * LANES : (b + 1) * LANES] = jnp.where(hit, 1.0, 0.0).astype(jnp.bfloat16)

        def main(accs):
            acc = {(q, m, c): accs[m][q * chunks + c] for q in mxus for m in mxus for c in range(chunks)}
            ent = {(m, c): accs[m][2 * chunks + c] for m in mxus for c in range(chunks)}

            def matmul(r, p, k):
                deep_k = slice(k * step, (k + 1) * step)
                for m in mxus:
                    cols = slice((2 * p + m) * step, (2 * p + m + 1) * step)
                    pltpu.matmul_push_rhs(sens_ref[deep_k, cols], 0, m)
                for c in range(chunks):
                    at = pl.ds(r * step + c * ch, ch)
                    lhs = rows_ref[at, deep_k]
                    for m in mxus:
                        pltpu.matmul_acc_lhs(acc[p, m, c], lhs, 0 if c == 0 else None)

            left = (iota((ch, LANES), 1) & (INSTR - 1)) < INSTR // 2

            def epilogue(p, c):
                tiles = []
                for m in mxus:
                    cols = slice((2 * p + m) * step, (2 * p + m + 1) * step)
                    value = pltpu.matmul_pop(acc[p, m, c])
                    inst = notional_ref[:, cols] * (
                        softplus2(value * LOG2E + money_ref[:, cols]) - base_ref[:, cols]
                    )
                    a, b = inst[:, 0:LANES], inst[:, LANES:]
                    a = a + pltpu.roll(a, LANES - INSTR // 2, 1)
                    b = b + pltpu.roll(b, INSTR // 2, 1)
                    tiles.append(jnp.where(left, a, b))
                hi, lo = split_bf16(jnp.concatenate(tiles, axis=1))
                halves_ref[0, c * ch : (c + 1) * ch, :] = hi
                halves_ref[1, c * ch : (c + 1) * ch, :] = lo

            def entities(p):
                for m in mxus:
                    pltpu.matmul_push_rhs(ent_w[p * step : (p + 1) * step, :], 1, m)
                for c in range(chunks):
                    for m in mxus:
                        part = halves_ref[m, c * ch : (c + 1) * ch, :]
                        pltpu.matmul_acc_lhs(ent[m, c], part, 1 if c == 0 else None)

            def collect(r):
                for c in range(chunks):
                    at = pl.ds(r * step + c * ch, ch)
                    sums = pltpu.matmul_pop(ent[0, c]) + pltpu.matmul_pop(ent[1, c])
                    res_ref[at, 0:LANES] = sums[:, 0:LANES]
                    valid = iota((ch, LANES), 0) + (r * step + c * ch) < count
                    res_ref[at, LANES:] = jnp.where(valid, sums[:, LANES:], LOW)

            count = count_ref[0]
            lane8 = iota((8, LANES), 1)
            sub = iota((8, LANES), 0)
            lists = TOPK // LANES
            per8 = LANES // 8

            def as_row(col):
                line = jnp.zeros((8, LANES), jnp.float32)
                for g in range(per8):
                    line = line + jnp.where(lane8 == sub + 8 * g, col(8 * g), 0.0)
                return jnp.broadcast_to(jnp.sum(line, axis=0, keepdims=True), (8, LANES))

            def losses(block):
                return lambda at: res_ref[block * LANES + at : block * LANES + at + 8, LANES:]

            def join(r, places):
                cols = [
                    losses(q) if r == 1 else (lambda at, q=q: best_ref[q * LANES + at : q * LANES + at + 8, :])
                    for q in range(lists)
                ]
                fresh = step // LANES
                cols += [losses(r * fresh + q) for q in range(fresh)]
                for b in range(0 if r == 1 else lists, lists + fresh):
                    line_ref[8 * b : 8 * b + 8, :] = as_row(cols[b])
                out = [jnp.zeros((8, LANES), jnp.float32) for _ in range(lists)]
                for a in range(lists + fresh):
                    known = a < lists and r > 1
                    for g in range(per8):
                        col = cols[a](8 * g)
                        ahead = jnp.zeros((8, LANES), jnp.float32)
                        for b in range(lists if known else 0, lists + fresh):
                            row = line_ref[8 * b : 8 * b + 8, :]
                            if b < a:
                                first = row >= col
                            elif b > a:
                                first = row > col
                            else:
                                first = (row > col) | ((row == col) & (lane8 < sub + 8 * g))
                            ahead = ahead + jnp.where(first, 1.0, 0.0)
                        rank = jnp.broadcast_to(jnp.sum(ahead, axis=1, keepdims=True), (8, LANES))
                        if known:
                            rank = rank + (sub + (a * LANES + 8 * g)).astype(jnp.float32)
                        for h in range(lists):
                            out[h] = out[h] + jnp.where(rank == places[h], col, 0.0)
                return [jnp.sum(out[h], axis=0, keepdims=True) for h in range(lists)]

            upright = [(lane8 + h * LANES).astype(jnp.float32) for h in range(lists)]

            def compare(r):
                if r == 0:
                    return
                for h, line in enumerate(join(r, upright)):
                    line_ref[8 * h : 8 * h + 8, :] = jnp.broadcast_to(line, (8, LANES))
                    best_ref[h * LANES : (h + 1) * LANES, :] = jnp.transpose(
                        jnp.broadcast_to(line, (LANES, LANES))
                    )

            def unit(r, p):
                last = 1 - p
                for k in range(deep):
                    if r == 0 and k % (deep // 2) == 0:
                        q = k // (deep // 2)
                        if p == 0:
                            first_copy(q).wait()
                        sens_copy(p, q).wait()
                        if p == 0 and q == 1:
                            row_copy(1).start()
                        if p == 1 and q == 0:
                            for i in range(2, blocks):
                                row_copy(i).start()
                    matmul(r, p, k)
                    if r + p == 0 and k == 0:
                        tables()
                    if r + p == 0 and k % 2 == 1:
                        picks(k // 2)
                    if k % 2 == 1 and k // 2 < chunks and r + p > 0:
                        epilogue(last, k // 2)
                    if p == 1 and k == 1 and r > 0:
                        collect(r - 1)
                        compare(r - 1)
                if r + p > 0:
                    entities(last)

            def one_block(r):
                if r == 1:
                    row_copy(1).wait()
                if r == 2:
                    for i in range(2, blocks):
                        row_copy(i).wait()
                unit(r, 0)
                unit(r, 1)

            for r in range(blocks):
                one_block(r)
            cand_accs = [accs[m][:chunks] + accs[m][3 * chunks :] for m in mxus]

            def route(k):
                hi, lo = split_bf16(res_ref[k * step : (k + 1) * step, 0:LANES])
                both = jnp.concatenate([hi, lo], axis=1)
                for m in mxus:
                    pltpu.matmul_push_rhs(both, 0, m)
                for c in range(2 * chunks):
                    for m in mxus:
                        at = m * (cands // 2) + c * ch
                        lhs = pick_ref[at : at + ch, k * step : (k + 1) * step]
                        pltpu.matmul_acc_lhs(cand_accs[m][c], lhs, 0 if c == 0 else None)

            for k in range(2):
                route(k)
            for c in range(chunks):
                epilogue(1, c)
            entities(1)
            for k in range(2, blocks - 1):
                route(k)
            collect(blocks - 1)
            route(blocks - 1)
            flip = lax.axis_index(axes[0]) >= devices // 2
            places = [jnp.where(flip, TOPK - 1 - place, place) for place in upright]
            for h, line in enumerate(join(blocks - 1, places)):
                out_ref[:, :, h * LANES : (h + 1) * LANES] = jnp.broadcast_to(
                    line[None], (devices, 1, LANES)
                )
            per = cands // devices
            keep = iota((1, per, LANES), 2) // ENT == iota((1, per, LANES), 1)
            for m in mxus:
                for c in range(2 * chunks):
                    got = pltpu.matmul_pop(cand_accs[m][c])
                    got = (got[:, 0:LANES] + got[:, LANES:]).reshape(ch // per, per, LANES)
                    at = (m * (cands // 2) + c * ch) // per
                    out_ref[at : at + ch // per, :, TOPK:] = jnp.sum(
                        jnp.where(keep, got, 0.0), axis=1, keepdims=True
                    )

        accs = [[pltpu.ACC(m)((ch, step), jnp.float32) for _ in range(4 * chunks)] for m in mxus]
        pl.run_scoped(lambda *refs: main((refs[: 4 * chunks], refs[4 * chunks :])), *accs[0], *accs[1])

    pl.run_scoped(
        whole,
        pltpu.VMEM(shocks_hbm.shape, jnp.bfloat16),
        pltpu.VMEM(sens_hbm.shape, jnp.bfloat16),
    )


def merge_kernel(in_ref, own_ref, send_ref):
    devices = in_ref.shape[0]
    lists = in_ref[...].reshape(devices, in_ref.shape[2])
    sums = jnp.sum(lists[:, TOPK:], axis=0, keepdims=True)
    own_ref[:, TOPK:] = sums
    send_ref[:, TOPK:] = sums

    lists = jnp.concatenate([lists[:, 0:TOPK]] * (LANES // devices), axis=0)
    turned = [jnp.transpose(lists[:, h * LANES : (h + 1) * LANES]) for h in range(TOPK // LANES)]
    per = LANES // 8
    x = [turned[g // per][8 * (g % per) : 8 * (g % per) + 8] for g in range(TOPK // 8)]
    lane = iota((8, LANES), 1)
    sub = iota((8, LANES), 0)

    def ordered(x):
        gap = len(x) // 2
        while gap:
            new = list(x)
            for g in range(len(x)):
                if not g & gap:
                    new[g] = jnp.maximum(x[g], x[g + gap])
                    new[g + gap] = jnp.minimum(x[g], x[g + gap])
            x, gap = new, gap // 2
        for gap in (4, 2, 1):
            upper = (sub & gap) == 0
            new = []
            for v in x:
                other = pltpu.roll(v, 8 - gap, 0)
                low = pltpu.roll(jnp.minimum(v, other), gap, 0)
                new.append(jnp.where(upper, jnp.maximum(v, other), low))
            x = new
        return x

    gap = devices // 2
    while gap:
        x = [jnp.maximum(v, pltpu.roll(v, gap, 1)) for v in x]
        gap //= 2
        if gap:
            sign = jnp.where((lane & gap) == 0, 1.0, -1.0)
            x = [v * sign for v in ordered([v * sign for v in x])]
    x = ordered(x)
    for h in range(TOPK // LANES):
        fall = rise = jnp.zeros((8, LANES), jnp.float32)
        for g in range(per):
            v = x[h * per + g]
            fall = fall + jnp.where(lane == sub + 8 * g, v, 0.0)
            rise = rise + jnp.where(lane == LANES - 1 - sub - 8 * g, v, 0.0)
        own_ref[:, h * LANES : (h + 1) * LANES] = jnp.sum(fall, axis=0, keepdims=True)
        other = TOPK - (h + 1) * LANES
        send_ref[:, other : other + LANES] = jnp.sum(rise, axis=0, keepdims=True)


def join_kernel(core_axis, own_ref, came_ref, tail_ref, cand_ref):
    total = own_ref[:, TOPK:] + came_ref[:, TOPK:]
    per = LANES // lax.axis_size(core_axis)
    total = jnp.where(lax.axis_index(core_axis) == 0, total, pltpu.roll(total, per, 1))
    spread = jnp.where(iota((8, LANES), 1) // ENT == iota((8, LANES), 0), total, 0.0)
    for d in (32, 16, 8):
        spread = spread + pltpu.roll(spread, LANES - d, 1)
    cand_ref[...] = spread[:, 0:ENT]

    parts = range(TOPK // LANES)
    rows = []
    cols = []
    for h in parts:
        span = slice(h * LANES, (h + 1) * LANES)
        rows.append(jnp.broadcast_to(jnp.maximum(own_ref[:, span], came_ref[:, span]), (LANES, LANES)))
        cols.append(jnp.transpose(rows[h]))
    before = iota((LANES, LANES), 1) < iota((LANES, LANES), 0)
    lines = [jnp.zeros((1, LANES), jnp.float32) for _ in parts]
    for a in parts:
        ahead = jnp.zeros((LANES, LANES), jnp.float32)
        for b in parts:
            if b < a:
                first = rows[b] >= cols[a]
            elif b > a:
                first = rows[b] > cols[a]
            else:
                first = (rows[b] > cols[a]) | ((rows[b] == cols[a]) & before)
            ahead = ahead + jnp.where(first, 1.0, 0.0)
        rank = jnp.sum(ahead, axis=1, keepdims=True)
        for h in parts:
            place = (iota((LANES, LANES), 1) + h * LANES).astype(jnp.float32)
            picked = jnp.where(rank == place, cols[a], 0.0)
            lines[h] = lines[h] + jnp.sum(picked, axis=0, keepdims=True)
    for h in parts:
        tail_ref[:, h * LANES : (h + 1) * LANES] = lines[h]


def price_call(slots, factors, instruments, cands, axes, devices):
    return pl.pallas_call(
        functools.partial(price_kernel, axes, devices),
        out_shape=jax.ShapeDtypeStruct((devices, 1, TOPK + LANES), jnp.float32),
        in_specs=[SMEM] + [HBM] * 6,
        out_specs=VMEM,
        scratch_shapes=[
            pltpu.VMEM((instruments // 2, 2 * LANES), jnp.bfloat16),
            pltpu.VMEM((slots, 2 * LANES), jnp.float32),
            pltpu.VMEM((cands, slots), jnp.bfloat16),
            pltpu.VMEM((cands, LANES), jnp.float32),
            pltpu.VMEM((2, 256, 256), jnp.bfloat16),
            pltpu.VMEM((1, cands), jnp.int32),
            pltpu.VMEM((1, instruments), jnp.float32),
            pltpu.VMEM((1, instruments), jnp.float32),
            pltpu.VMEM((1, instruments), jnp.float32),
            pltpu.VMEM((32, LANES), jnp.float32),
            pltpu.VMEM((TOPK, LANES), jnp.float32),
            pltpu.SMEM((K,), jnp.int32),
            pltpu.SemaphoreType.DMA((slots // 256 + 1,)),
            pltpu.SemaphoreType.DMA((instruments // 512, 2)),
            pltpu.SemaphoreType.DMA((4,)),
        ],
        compiler_params=pltpu.CompilerParams(vmem_limit_bytes=PRICE_VMEM),
        name="price",
    )


def body(shocks, factor_sens, notional, moneyness, desk_entity, scenario_counts, candidate_ids):
    slots, factors = shocks.shape
    instruments = factor_sens.shape[1]
    cands = candidate_ids.shape[0]
    chips, cores = lax.axis_size("chip"), lax.axis_size("core")
    args = (
        scenario_counts,
        desk_entity,
        candidate_ids.reshape(1, cands),
        notional.reshape(1, instruments),
        moneyness.reshape(1, instruments),
        shocks,
        factor_sens,
    )
    args = args[:1] + tuple(pltpu.with_memory_space_constraint(a, pltpu.HBM) for a in args[1:])
    price = price_call(slots, factors, instruments, cands, ("chip", "core"), chips)
    got = lax.all_to_all(price(*args), "chip", 0, 0, tiled=True)
    line = jax.ShapeDtypeStruct((1, TOPK + LANES), jnp.float32)
    own, send = pl.pallas_call(
        merge_kernel,
        out_shape=[line, line],
        in_specs=[VMEM],
        out_specs=[VMEM, VMEM],
        compiler_params=pltpu.CompilerParams(vmem_limit_bytes=MERGE_VMEM),
        name="merge",
    )(got)
    came = lax.ppermute(send, "core", [(0, 1), (1, 0)])
    tail, cand = pl.pallas_call(
        functools.partial(join_kernel, "core"),
        out_shape=[
            jax.ShapeDtypeStruct((1, TOPK), jnp.float32),
            jax.ShapeDtypeStruct((cands // (chips * cores), ENT), jnp.float32),
        ],
        in_specs=[VMEM, VMEM],
        out_specs=[VMEM, VMEM],
        compiler_params=pltpu.CompilerParams(vmem_limit_bytes=MERGE_VMEM),
        name="join",
    )(own, came)
    return tail.reshape(TOPK), cand


def solution(mesh):
    groups, scen = mesh.shape["grp"], mesh.shape["scen"]
    finer = Mesh(mesh.devices.reshape(groups, scen // 2, 2), ("grp", "chip", "core"))
    every = ("grp", "chip", "core")
    return jax.shard_map(
        body,
        mesh=finer,
        in_specs=(P(every, None), P(), P(), P(), P(), P(every), P("grp")),
        out_specs=(P("grp"), P(every, None)),
        check_vma=False,
    )
```

```python
import functools

import jax
import jax.numpy as jnp
from jax import lax
from jax.experimental import pallas as pl
from jax.experimental.pallas import tpu as pltpu
from jax.sharding import Mesh
from jax.sharding import PartitionSpec as P

K = 64
INSTR = 16
ENT = 8
TOPK = 256
LANES = 128
LOG2E = 1.4426950408889634
LN2 = 0.6931471805599453
LOW = -1e30
DELAY = 250

VMEM = pl.BlockSpec(memory_space=pltpu.VMEM)
SMEM = pl.BlockSpec(memory_space=pltpu.SMEM)
HBM = pl.BlockSpec(memory_space=pltpu.HBM)
PRICE_VMEM = 24 << 20
MERGE_VMEM = 8 << 20


def softplus2(t):
    top = jnp.maximum(t, 0.0)
    return top + jnp.log2(1.0 + jnp.exp2(t - top - top))


def iota(shape, dim):
    return lax.broadcasted_iota(jnp.int32, shape, dim)


def split_bf16(x):
    hi = x.astype(jnp.bfloat16)
    return hi, (x - hi.astype(jnp.float32)).astype(jnp.bfloat16)


def price_kernel(
    axes, devices, count_ref, desk_hbm, ids_hbm, notional_hbm, money_hbm, shocks_hbm, sens_hbm,
    out_ref, ent_w, res_ref, pick_ref, idc_ref, halves_ref, ids_ref, notional_ref,
    money_ref, base_ref, line_ref, best_ref, desk_ref, row_sems, sens_sems, small_sems,
):
    def whole(rows_ref, sens_ref):
        slots, factors = shocks_hbm.shape
        instruments = sens_hbm.shape[1]
        cands = ids_ref.shape[1]
        step = 256
        blocks = slots // step
        pairs = instruments // (2 * step)
        deep = factors // step
        ch = 64
        chunks = step // ch
        mxus = (0, 1)

        half = factors // 2

        def row_copy(i):
            part = pl.ds(i * step, step)
            return pltpu.make_async_copy(shocks_hbm.at[part], rows_ref.at[part], row_sems.at[i])

        def first_copy(q):
            part = (pl.ds(0, step), pl.ds(q * half, half))
            return pltpu.make_async_copy(shocks_hbm.at[part], rows_ref.at[part], row_sems.at[blocks * q])

        def sens_copy(p, q):
            part = (pl.ds(q * half, half), pl.ds(p * 2 * step, 2 * step))
            return pltpu.make_async_copy(sens_hbm.at[part], sens_ref.at[part], sens_sems.at[p, q])

        small = [
            pltpu.make_async_copy(a, b, small_sems.at[n])
            for n, (a, b) in enumerate(
                (
                    (desk_hbm, desk_ref),
                    (ids_hbm, ids_ref),
                    (notional_hbm, notional_ref),
                    (money_hbm, money_ref),
                )
            )
        ]
        for copy in small:
            copy.start()
        first_copy(0).start()
        sens_copy(0, 0).start()
        pl.delay(DELAY)
        first_copy(1).start()
        sens_copy(0, 1).start()
        pl.delay(DELAY)
        for p in range(1, pairs):
            for q in range(2):
                sens_copy(p, q).start()
        me = lax.axis_index(axes[0]) * lax.axis_size(axes[1]) + lax.axis_index(axes[1])

        def tables():
            for copy in small:
                copy.wait()
            lane = iota((INSTR, LANES), 1)
            upper = iota((INSTR, LANES), 0) < INSTR // 2
            per_tile = LANES // INSTR
            for k in range(instruments // (2 * INSTR)):
                desk = k // per_tile * 2 * per_tile + k % per_tile
                entity = jnp.where(upper, desk_ref[desk], desk_ref[desk + per_tile])
                hit = (lane & (ENT - 1)) == entity
                ent_w[pl.ds(k * INSTR, INSTR), 0:LANES] = jnp.where(hit, -1.0, 0.0).astype(jnp.bfloat16)
            ent_w[:, LANES:] = jnp.full((instruments // 2, LANES), -1.0, jnp.bfloat16)
            money_ref[...] = money_ref[...] * LOG2E
            base_ref[...] = softplus2(money_ref[...])
            notional_ref[...] = notional_ref[...] * LN2
            local = (ids_ref[...] - me * slots).astype(jnp.float32)
            for b in range(cands // LANES):
                span = pl.ds(b * LANES, LANES)
                row = jnp.broadcast_to(local[:, b * LANES : (b + 1) * LANES], (LANES, LANES))
                idc_ref[span, :] = jnp.transpose(row)

        spot = iota((step, LANES), 1).astype(jnp.float32)
        def picks(i):
            mine = slice(i * step, (i + 1) * step)
            for b in range(slots // LANES):
                hit = idc_ref[mine, :] == spot + float(b * LANES)
                pick_ref[mine, b * LANES : (b + 1) * LANES] = jnp.where(hit, 1.0, 0.0).astype(jnp.bfloat16)

        def main(accs):
            acc = {(q, m, c): accs[m][q * chunks + c] for q in mxus for m in mxus for c in range(chunks)}
            ent = {(m, c): accs[m][2 * chunks + c] for m in mxus for c in range(chunks)}

            def matmul(r, p, k):
                deep_k = slice(k * step, (k + 1) * step)
                for m in mxus:
                    cols = slice((2 * p + m) * step, (2 * p + m + 1) * step)
                    pltpu.matmul_push_rhs(sens_ref[deep_k, cols], 0, m)
                for c in range(chunks):
                    at = pl.ds(r * step + c * ch, ch)
                    lhs = rows_ref[at, deep_k]
                    for m in mxus:
                        pltpu.matmul_acc_lhs(acc[p, m, c], lhs, 0 if c == 0 else None)

            left = (iota((ch, LANES), 1) & (INSTR - 1)) < INSTR // 2

            def epilogue(p, c):
                tiles = []
                for m in mxus:
                    cols = slice((2 * p + m) * step, (2 * p + m + 1) * step)
                    value = pltpu.matmul_pop(acc[p, m, c])
                    inst = notional_ref[:, cols] * (
                        softplus2(value * LOG2E + money_ref[:, cols]) - base_ref[:, cols]
                    )
                    a, b = inst[:, 0:LANES], inst[:, LANES:]
                    a = a + pltpu.roll(a, LANES - INSTR // 2, 1)
                    b = b + pltpu.roll(b, INSTR // 2, 1)
                    tiles.append(jnp.where(left, a, b))
                hi, lo = split_bf16(jnp.concatenate(tiles, axis=1))
                halves_ref[0, c * ch : (c + 1) * ch, :] = hi
                halves_ref[1, c * ch : (c + 1) * ch, :] = lo

            def entities(p):
                for m in mxus:
                    pltpu.matmul_push_rhs(ent_w[p * step : (p + 1) * step, :], 1, m)
                for c in range(chunks):
                    for m in mxus:
                        part = halves_ref[m, c * ch : (c + 1) * ch, :]
                        pltpu.matmul_acc_lhs(ent[m, c], part, 1 if c == 0 else None)

            def collect(r):
                for c in range(chunks):
                    at = pl.ds(r * step + c * ch, ch)
                    sums = pltpu.matmul_pop(ent[0, c]) + pltpu.matmul_pop(ent[1, c])
                    res_ref[at, 0:LANES] = sums[:, 0:LANES]
                    valid = iota((ch, LANES), 0) + (r * step + c * ch) < count
                    res_ref[at, LANES:] = jnp.where(valid, sums[:, LANES:], LOW)

            count = count_ref[0]
            lane8 = iota((8, LANES), 1)
            sub = iota((8, LANES), 0)
            lists = TOPK // LANES
            per8 = LANES // 8

            def as_row(col):
                line = jnp.zeros((8, LANES), jnp.float32)
                for g in range(per8):
                    line = line + jnp.where(lane8 == sub + 8 * g, col(8 * g), 0.0)
                return jnp.broadcast_to(jnp.sum(line, axis=0, keepdims=True), (8, LANES))

            def losses(block):
                return lambda at: res_ref[block * LANES + at : block * LANES + at + 8, LANES:]

            def join(r, places):
                cols = [
                    losses(q) if r == 1 else (lambda at, q=q: best_ref[q * LANES + at : q * LANES + at + 8, :])
                    for q in range(lists)
                ]
                fresh = step // LANES
                cols += [losses(r * fresh + q) for q in range(fresh)]
                for b in range(0 if r == 1 else lists, lists + fresh):
                    line_ref[8 * b : 8 * b + 8, :] = as_row(cols[b])
                out = [jnp.zeros((8, LANES), jnp.float32) for _ in range(lists)]
                for a in range(lists + fresh):
                    known = a < lists and r > 1
                    for g in range(per8):
                        col = cols[a](8 * g)
                        ahead = jnp.zeros((8, LANES), jnp.float32)
                        for b in range(lists if known else 0, lists + fresh):
                            row = line_ref[8 * b : 8 * b + 8, :]
                            if b < a:
                                first = row >= col
                            elif b > a:
                                first = row > col
                            else:
                                first = (row > col) | ((row == col) & (lane8 < sub + 8 * g))
                            ahead = ahead + jnp.where(first, 1.0, 0.0)
                        rank = jnp.broadcast_to(jnp.sum(ahead, axis=1, keepdims=True), (8, LANES))
                        if known:
                            rank = rank + (sub + (a * LANES + 8 * g)).astype(jnp.float32)
                        for h in range(lists):
                            out[h] = out[h] + jnp.where(rank == places[h], col, 0.0)
                return [jnp.sum(out[h], axis=0, keepdims=True) for h in range(lists)]

            upright = [(lane8 + h * LANES).astype(jnp.float32) for h in range(lists)]

            def compare(r):
                if r == 0:
                    return
                for h, line in enumerate(join(r, upright)):
                    line_ref[8 * h : 8 * h + 8, :] = jnp.broadcast_to(line, (8, LANES))
                    best_ref[h * LANES : (h + 1) * LANES, :] = jnp.transpose(
                        jnp.broadcast_to(line, (LANES, LANES))
                    )

            def unit(r, p):
                last = 1 - p
                for k in range(deep):
                    if r == 0 and k % (deep // 2) == 0:
                        q = k // (deep // 2)
                        if p == 0:
                            first_copy(q).wait()
                        sens_copy(p, q).wait()
                        if p == 0 and q == 1:
                            row_copy(1).start()
                        if p == 1 and q == 0:
                            for i in range(2, blocks):
                                row_copy(i).start()
                    matmul(r, p, k)
                    if r + p == 0 and k == 0:
                        tables()
                    if r + p == 0 and k % 2 == 1:
                        picks(k // 2)
                    if k % 2 == 1 and k // 2 < chunks and r + p > 0:
                        epilogue(last, k // 2)
                    if p == 1 and k == 1 and r > 0:
                        collect(r - 1)
                        compare(r - 1)
                if r + p > 0:
                    entities(last)

            def one_block(r):
                if r == 1:
                    row_copy(1).wait()
                if r == 2:
                    for i in range(2, blocks):
                        row_copy(i).wait()
                unit(r, 0)
                unit(r, 1)

            for r in range(blocks):
                one_block(r)
            cand_accs = [accs[m][:chunks] + accs[m][3 * chunks :] for m in mxus]

            def route(k):
                hi, lo = split_bf16(res_ref[k * step : (k + 1) * step, 0:LANES])
                both = jnp.concatenate([hi, lo], axis=1)
                for m in mxus:
                    pltpu.matmul_push_rhs(both, 0, m)
                for c in range(2 * chunks):
                    for m in mxus:
                        at = m * (cands // 2) + c * ch
                        lhs = pick_ref[at : at + ch, k * step : (k + 1) * step]
                        pltpu.matmul_acc_lhs(cand_accs[m][c], lhs, 0 if c == 0 else None)

            for k in range(2):
                route(k)
            for c in range(chunks):
                epilogue(1, c)
            entities(1)
            for k in range(2, blocks - 1):
                route(k)
            collect(blocks - 1)
            route(blocks - 1)
            flip = lax.axis_index(axes[0]) >= devices // 2
            places = [jnp.where(flip, TOPK - 1 - place, place) for place in upright]
            for h, line in enumerate(join(blocks - 1, places)):
                out_ref[:, :, h * LANES : (h + 1) * LANES] = jnp.broadcast_to(
                    line[None], (devices, 1, LANES)
                )
            per = cands // devices
            keep = iota((1, per, LANES), 2) // ENT == iota((1, per, LANES), 1)
            for m in mxus:
                for c in range(2 * chunks):
                    got = pltpu.matmul_pop(cand_accs[m][c])
                    got = (got[:, 0:LANES] + got[:, LANES:]).reshape(ch // per, per, LANES)
                    at = (m * (cands // 2) + c * ch) // per
                    out_ref[at : at + ch // per, :, TOPK:] = jnp.sum(
                        jnp.where(keep, got, 0.0), axis=1, keepdims=True
                    )

        accs = [[pltpu.ACC(m)((ch, step), jnp.float32) for _ in range(4 * chunks)] for m in mxus]
        pl.run_scoped(lambda *refs: main((refs[: 4 * chunks], refs[4 * chunks :])), *accs[0], *accs[1])

    pl.run_scoped(
        whole,
        pltpu.VMEM(shocks_hbm.shape, jnp.bfloat16),
        pltpu.VMEM(sens_hbm.shape, jnp.bfloat16),
    )


def merge_kernel(in_ref, own_ref, send_ref):
    devices = in_ref.shape[0]
    lists = in_ref[...].reshape(devices, in_ref.shape[2])
    sums = jnp.sum(lists[:, TOPK:], axis=0, keepdims=True)
    own_ref[:, TOPK:] = sums
    send_ref[:, TOPK:] = sums

    lists = jnp.concatenate([lists[:, 0:TOPK]] * (LANES // devices), axis=0)
    turned = [jnp.transpose(lists[:, h * LANES : (h + 1) * LANES]) for h in range(TOPK // LANES)]
    per = LANES // 8
    x = [turned[g // per][8 * (g % per) : 8 * (g % per) + 8] for g in range(TOPK // 8)]
    lane = iota((8, LANES), 1)
    sub = iota((8, LANES), 0)

    def ordered(x):
        gap = len(x) // 2
        while gap:
            new = list(x)
            for g in range(len(x)):
                if not g & gap:
                    new[g] = jnp.maximum(x[g], x[g + gap])
                    new[g + gap] = jnp.minimum(x[g], x[g + gap])
            x, gap = new, gap // 2
        for gap in (4, 2, 1):
            upper = (sub & gap) == 0
            new = []
            for v in x:
                other = pltpu.roll(v, 8 - gap, 0)
                low = jnp.minimum(v, other)
                if gap != 4:
                    low = pltpu.roll(low, gap, 0)
                new.append(jnp.where(upper, jnp.maximum(v, other), low))
            x = new
        return x

    gap = devices // 2
    while gap:
        x = [jnp.maximum(v, pltpu.roll(v, gap, 1)) for v in x]
        gap //= 2
        if gap:
            sign = jnp.where((lane & gap) == 0, 1.0, -1.0)
            x = [v * sign for v in ordered([v * sign for v in x])]
    x = ordered(x)
    for h in range(TOPK // LANES):
        fall = rise = jnp.zeros((8, LANES), jnp.float32)
        for g in range(per):
            v = x[h * per + g]
            fall = fall + jnp.where(lane == sub + 8 * g, v, 0.0)
            rise = rise + jnp.where(lane == LANES - 1 - sub - 8 * g, v, 0.0)
        own_ref[:, h * LANES : (h + 1) * LANES] = jnp.sum(fall, axis=0, keepdims=True)
        other = TOPK - (h + 1) * LANES
        send_ref[:, other : other + LANES] = jnp.sum(rise, axis=0, keepdims=True)


def join_kernel(core_axis, own_ref, came_ref, tail_ref, cand_ref):
    total = own_ref[:, TOPK:] + came_ref[:, TOPK:]
    per = LANES // lax.axis_size(core_axis)
    total = jnp.where(lax.axis_index(core_axis) == 0, total, pltpu.roll(total, per, 1))
    spread = jnp.where(iota((8, LANES), 1) // ENT == iota((8, LANES), 0), total, 0.0)
    for d in (32, 16, 8):
        spread = spread + pltpu.roll(spread, LANES - d, 1)
    cand_ref[...] = spread[:, 0:ENT]

    parts = range(TOPK // LANES)
    rows = []
    cols = []
    for h in parts:
        span = slice(h * LANES, (h + 1) * LANES)
        rows.append(jnp.broadcast_to(jnp.maximum(own_ref[:, span], came_ref[:, span]), (LANES, LANES)))
        cols.append(jnp.transpose(rows[h]))
    before = iota((LANES, LANES), 1) < iota((LANES, LANES), 0)
    lines = [jnp.zeros((1, LANES), jnp.float32) for _ in parts]
    for a in parts:
        ahead = jnp.zeros((LANES, LANES), jnp.float32)
        for b in parts:
            if b < a:
                first = rows[b] >= cols[a]
            elif b > a:
                first = rows[b] > cols[a]
            else:
                first = (rows[b] > cols[a]) | ((rows[b] == cols[a]) & before)
            ahead = ahead + jnp.where(first, 1.0, 0.0)
        rank = jnp.sum(ahead, axis=1, keepdims=True)
        for h in parts:
            place = (iota((LANES, LANES), 1) + h * LANES).astype(jnp.float32)
            picked = jnp.where(rank == place, cols[a], 0.0)
            lines[h] = lines[h] + jnp.sum(picked, axis=0, keepdims=True)
    for h in parts:
        tail_ref[:, h * LANES : (h + 1) * LANES] = lines[h]


def price_call(slots, factors, instruments, cands, axes, devices):
    return pl.pallas_call(
        functools.partial(price_kernel, axes, devices),
        out_shape=jax.ShapeDtypeStruct((devices, 1, TOPK + LANES), jnp.float32),
        in_specs=[SMEM] + [HBM] * 6,
        out_specs=VMEM,
        scratch_shapes=[
            pltpu.VMEM((instruments // 2, 2 * LANES), jnp.bfloat16),
            pltpu.VMEM((slots, 2 * LANES), jnp.float32),
            pltpu.VMEM((cands, slots), jnp.bfloat16),
            pltpu.VMEM((cands, LANES), jnp.float32),
            pltpu.VMEM((2, 256, 256), jnp.bfloat16),
            pltpu.VMEM((1, cands), jnp.int32),
            pltpu.VMEM((1, instruments), jnp.float32),
            pltpu.VMEM((1, instruments), jnp.float32),
            pltpu.VMEM((1, instruments), jnp.float32),
            pltpu.VMEM((32, LANES), jnp.float32),
            pltpu.VMEM((TOPK, LANES), jnp.float32),
            pltpu.SMEM((K,), jnp.int32),
            pltpu.SemaphoreType.DMA((slots // 256 + 1,)),
            pltpu.SemaphoreType.DMA((instruments // 512, 2)),
            pltpu.SemaphoreType.DMA((4,)),
        ],
        compiler_params=pltpu.CompilerParams(vmem_limit_bytes=PRICE_VMEM),
        name="price",
    )


def body(shocks, factor_sens, notional, moneyness, desk_entity, scenario_counts, candidate_ids):
    slots, factors = shocks.shape
    instruments = factor_sens.shape[1]
    cands = candidate_ids.shape[0]
    chips, cores = lax.axis_size("chip"), lax.axis_size("core")
    args = (
        scenario_counts,
        desk_entity,
        candidate_ids.reshape(1, cands),
        notional.reshape(1, instruments),
        moneyness.reshape(1, instruments),
        shocks,
        factor_sens,
    )
    args = args[:1] + tuple(pltpu.with_memory_space_constraint(a, pltpu.HBM) for a in args[1:])
    price = price_call(slots, factors, instruments, cands, ("chip", "core"), chips)
    got = lax.all_to_all(price(*args), "chip", 0, 0, tiled=True)
    line = jax.ShapeDtypeStruct((1, TOPK + LANES), jnp.float32)
    own, send = pl.pallas_call(
        merge_kernel,
        out_shape=[line, line],
        in_specs=[VMEM],
        out_specs=[VMEM, VMEM],
        compiler_params=pltpu.CompilerParams(vmem_limit_bytes=MERGE_VMEM),
        name="merge",
    )(got)
    came = lax.ppermute(send, "core", [(0, 1), (1, 0)])
    tail, cand = pl.pallas_call(
        functools.partial(join_kernel, "core"),
        out_shape=[
            jax.ShapeDtypeStruct((1, TOPK), jnp.float32),
            jax.ShapeDtypeStruct((cands // (chips * cores), ENT), jnp.float32),
        ],
        in_specs=[VMEM, VMEM],
        out_specs=[VMEM, VMEM],
        compiler_params=pltpu.CompilerParams(vmem_limit_bytes=MERGE_VMEM),
        name="join",
    )(own, came)
    return tail.reshape(TOPK), cand


def solution(mesh):
    groups, scen = mesh.shape["grp"], mesh.shape["scen"]
    finer = Mesh(mesh.devices.reshape(groups, scen // 2, 2), ("grp", "chip", "core"))
    every = ("grp", "chip", "core")
    return jax.shard_map(
        body,
        mesh=finer,
        in_specs=(P(every, None), P(), P(), P(), P(), P(every), P("grp")),
        out_specs=(P("grp"), P(every, None)),
        check_vma=False,
    )
```
